128 devices in a mesh: col: 2 (over core), row: 64 (over z, y, x).
Axes of the slice: x: 4, y: 4, z: 4, core: 2. Of those that a mesh axis runs over, the one named last changes fastest.
Arguments:
- inter_mask: int32 [65536, 4096], P('row', 'col')
- emb_user: bfloat16 [65536, 64], P(('row', 'col'))
- emb_item: bfloat16 [4096, 64], P(('col', 'row'))
- triples: int32 [128, 3], replicated
Outputs:
- output 1: bfloat16 [65536, 64], P(('row', 'col'))
- output 2: bfloat16 [4096, 64], P(('col', 'row'))
- output 3: float32 [], replicated
All inputs are finite; a program needn't handle non-finite values.
Results may differ from the reference program's by a relative error of at most 0.00519882.
Values are sent between devices in bfloat16 or wider.
A program may use at most 1 GiB of HBM per device.

```python
import jax
import jax.numpy as jnp
from jax import lax

USERS = 65536
ITEMS = 4096
DIM = 64
LAYERS = 3
TRIPLES = 128
USER_DEGREE = 3


def draw_triples(trip_key):
    key_user, key_pos, key_neg = jax.random.split(trip_key, 3)
    row_pos = jnp.arange(TRIPLES)
    user_ids = jax.random.randint(key_user, (TRIPLES,), 0, USERS)
    pos_ids = jax.random.randint(key_pos, (TRIPLES,), 0, ITEMS)
    neg_ids = jax.random.randint(key_neg, (TRIPLES,), 0, ITEMS)
    user_ids = jnp.where(row_pos == 0, USERS - 1, jnp.where(row_pos == 1, 0, user_ids))
    pos_ids = jnp.where(row_pos == 0, ITEMS - 1, jnp.where(row_pos == 1, 0, pos_ids))
    neg_ids = jnp.where(row_pos == 0, 0, jnp.where(row_pos == 1, ITEMS - 1, neg_ids))
    return jnp.stack([user_ids, pos_ids, neg_ids], axis=1).astype(jnp.int32)


def setup_inputs(seed: int = 0) -> dict:
    base_key = jax.random.key(seed)
    key_mask, key_user, key_item, key_trip = jax.random.split(base_key, 4)
    raw_draw = jax.random.randint(key_mask, (USERS, ITEMS), 0, ITEMS)
    inter_mask = (raw_draw < USER_DEGREE).astype(jnp.int32)
    emb_user = jax.random.normal(key_user, (USERS, DIM), jnp.float32).astype(jnp.bfloat16)
    emb_item = jax.random.normal(key_item, (ITEMS, DIM), jnp.float32).astype(jnp.bfloat16)
    return {"inter_mask": inter_mask, "emb_user": emb_user, "emb_item": emb_item, "triples": draw_triples(key_trip)}


def reference(inter_mask, emb_user, emb_item, triples):
    deg_user = jnp.maximum(jnp.sum(inter_mask, axis=1), 1)
    deg_item = jnp.maximum(jnp.sum(inter_mask, axis=0), 1)
    scale_user = lax.rsqrt(deg_user.astype(jnp.float32))
    scale_item = lax.rsqrt(deg_item.astype(jnp.float32))
    norm_adj = (inter_mask.astype(jnp.float32) * scale_user[:, None] * scale_item[None, :]).astype(jnp.bfloat16)
    layer_user = emb_user
    layer_item = emb_item
    total_user = emb_user.astype(jnp.float32)
    total_item = emb_item.astype(jnp.float32)
    for layer_idx in range(LAYERS):
        next_user = jnp.dot(norm_adj, layer_item, preferred_element_type=jnp.float32).astype(jnp.bfloat16)
        next_item = lax.dot_general(norm_adj, layer_user, (((0,), (0,)), ((), ())), preferred_element_type=jnp.float32).astype(jnp.bfloat16)
        total_user = total_user + next_user.astype(jnp.float32)
        total_item = total_item + next_item.astype(jnp.float32)
        layer_user = next_user
        layer_item = next_item
    out_user = (total_user / (LAYERS + 1)).astype(jnp.bfloat16)
    out_item = (total_item / (LAYERS + 1)).astype(jnp.bfloat16)
    user_vec = jnp.take(out_user, triples[:, 0], axis=0).astype(jnp.float32)
    pos_vec = jnp.take(out_item, triples[:, 1], axis=0).astype(jnp.float32)
    neg_vec = jnp.take(out_item, triples[:, 2], axis=0).astype(jnp.float32)
    margin = jnp.sum(user_vec * pos_vec, axis=1) - jnp.sum(user_vec * neg_vec, axis=1)
    bpr_loss = jnp.mean(jax.nn.softplus(-margin))
    return out_user, out_item, bpr_loss
```

```python
import jax
import jax.numpy as jnp
from jax import lax
from jax.experimental import pallas as pl
from jax.experimental.pallas import tpu as pltpu
from jax.sharding import PartitionSpec as P

F32 = jnp.float32
BF16 = jnp.bfloat16
LANES = 128


def solution(mesh):
    rows_n = mesh.shape["row"]
    side = round(rows_n ** (1 / 3))
    plane = side * side

    def kernel(m_hbm, eu_hbm, ei_hbm, trip_hbm, ou_hbm, oi_hbm, loss_hbm,
               m32, a, at, cacc, trip, deg, usum, suc, svr, svc, e0, e0d, eup, eu0,
               up1, ur1, part, r12, panel, up3, ur3, eu23, eud, p3, r3, outd, outu, outi,
               ea, ear1, ea1, ear2, xs, xd, lossv,
               m_sem, in_sem, out_sem,
               deg_s, deg_r, e0_s, e0_r, eu0_s, eu0_r, us_s, us_r, u1_s, u1_r, rs_s, rs_r,
               ag_s, ag_r, u3_s, u3_r, r3_s, r3_r, ea1_s, ea1_r, ea2_s, ea2_r, xs_s, xs_r, xd_s, xd_r):
        me = lax.axis_index("row")
        col = lax.axis_index("col")
        mx = me % side
        my = (me // side) % side
        mz = me // plane
        users, items = a.shape
        half = users // 2
        shard = items // rows_n
        ublk = users // LANES
        iblk = items // LANES

        def peer(o):
            px = (mx + o % side) % side
            py = (my + (o // side) % side) % side
            pz = (mz + o // plane) % side
            return px + side * py + plane * pz

        def dup_lo(v):
            lane = lax.broadcasted_iota(jnp.int32, v.shape, v.ndim - 1)
            return jnp.where(lane < 64, v, pltpu.roll(v, 64, v.ndim - 1))

        def dup_hi(v):
            lane = lax.broadcasted_iota(jnp.int32, v.shape, v.ndim - 1)
            return jnp.where(lane < 64, pltpu.roll(v, 64, v.ndim - 1), v)

        def each_peer(fn):
            def body(o, carry):
                fn(peer(o))
                return carry
            lax.fori_loop(1, rows_n, body, 0)

        def send(src, dst, ssem, rsem, where):
            pltpu.make_async_remote_copy(src_ref=src, dst_ref=dst, send_sem=ssem, recv_sem=rsem,
                                         device_id=where).start()

        def wait_bytes(ref, sem):
            pltpu.make_async_copy(ref, ref, sem).wait()

        m_copies = []
        for b in range(ublk):
            blk = pl.ds(b * LANES, LANES)
            m_copies.append(pltpu.make_async_copy(m_hbm.at[blk], m32.at[blk], m_sem.at[b]))
            m_copies[-1].start()
        own_u = pl.ds(pl.multiple_of(col * half, half), half)
        own_i = pl.ds(pl.multiple_of(me * shard, shard), shard)
        c_eu = pltpu.make_async_copy(eu_hbm, eu0.at[own_u], in_sem.at[0])
        c_ei = pltpu.make_async_copy(ei_hbm, e0.at[own_i], in_sem.at[1])
        c_tr = pltpu.make_async_copy(trip_hbm, trip, in_sem.at[2])
        c_eu.start()
        c_ei.start()
        c_tr.start()
        barrier = pltpu.get_barrier_semaphore()
        each_peer(lambda p: pl.semaphore_signal(barrier, inc=1, device_id={"row": p}))
        pl.semaphore_signal(barrier, inc=1, device_id={"col": 1 - col})

        cacc[...] = jnp.zeros_like(cacc)
        for b in range(ublk):
            m_copies[b].wait()

            def colsum(i, carry):
                r = pl.ds(pl.multiple_of(b * LANES + i * 32, 32), 32)
                v = m32[r, :].astype(F32)
                cacc[...] += jnp.sum(v.reshape(4, 8, items), axis=0)
                a[r, :] = v.astype(BF16)
                return carry
            lax.fori_loop(0, LANES // 32, colsum, 0)
        dsum = jnp.sum(cacc[...], axis=0, keepdims=True)
        for i in range(iblk):
            deg[me, i:i + 1, :] = dsum[:, i * LANES:(i + 1) * LANES]
        c_eu.wait()
        c_ei.wait()
        c_tr.wait()
        pl.semaphore_wait(barrier, rows_n)
        each_peer(lambda p: send(deg.at[me], deg.at[me], deg_s, deg_r, {"row": p}))
        each_peer(lambda p: send(e0.at[own_i], e0.at[own_i], e0_s, e0_r, {"row": p}))
        send(eu0.at[own_u], eu0.at[own_u], eu0_s, eu0_r, {"col": 1 - col})

        ones = jnp.ones((items, LANES), BF16)
        for b in range(ublk):
            rsum = jnp.dot(a[b * LANES:(b + 1) * LANES, :], ones, preferred_element_type=F32)
            usum[col, b:b + 1, :] = jnp.transpose(rsum)[0:1, :]
        send(usum.at[col], usum.at[col], us_s, us_r, {"col": 1 - col})

        def flip(i, carry):
            c = pl.ds(pl.multiple_of(i * LANES, LANES), LANES)
            at[c, :] = jnp.transpose(a[:, c])
            return carry
        lax.fori_loop(0, iblk, flip, 0)
        wait_bytes(usum.at[0], us_r)
        su = lax.rsqrt(jnp.maximum(usum[0] + usum[1], 1.0))
        for b in range(ublk):
            suc[b * LANES:(b + 1) * LANES, :] = jnp.transpose(jnp.broadcast_to(su[b:b + 1, :], (LANES, LANES)))
        wait_bytes(eu0.at[pl.ds(0, half)], eu0_r)
        eup[:, 0:64] = eu0[...]
        wait_bytes(e0.at[pl.ds(0, (rows_n - 1) * shard)], e0_r)
        e0d[...] = jnp.concatenate([e0[...], e0[...]], axis=1)

        wait_bytes(deg.at[pl.ds(0, rows_n - 1)], deg_r)
        svr[...] = lax.rsqrt(jnp.maximum(jnp.sum(deg[...], axis=0), 1.0))

        def scale_a(i, carry):
            c = pl.ds(pl.multiple_of(i * LANES, LANES), LANES)
            a[:, c] = (a[:, c].astype(F32) * suc[...] * svr[pl.ds(i, 1), :]).astype(BF16)
            return carry
        lax.fori_loop(0, iblk, scale_a, 0)

        lane = lax.broadcasted_iota(jnp.int32, (half, LANES), 1)
        top = jnp.dot(a[0:half, :], e0d[...], preferred_element_type=F32)
        bot = jnp.dot(a[half:users, :], e0d[...], preferred_element_type=F32)
        up1[...] = jnp.where(lane < 64, top, bot)
        send(up1, ur1, u1_s, u1_r, {"col": 1 - col})

        def scale_at(i, carry):
            r = pl.ds(pl.multiple_of(i * LANES, LANES), LANES)
            sv = jnp.transpose(jnp.broadcast_to(svr[pl.ds(i, 1), :], (LANES, LANES)))
            for b in range(ublk):
                c = slice(b * LANES, (b + 1) * LANES)
                at[r, c] = (at[r, c].astype(F32) * su[b:b + 1, :] * sv).astype(BF16)
            return carry
        lax.fori_loop(0, iblk, scale_at, 0)
        wait_bytes(ur1, u1_r)
        s1 = up1[...] + ur1[...]
        eup[0:half, 64:128] = pltpu.roll(s1, 64, 1)[:, 64:128].astype(BF16)
        eup[half:users, 64:128] = s1[:, 64:128].astype(BF16)

        step = 512

        def mm2(i, carry):
            r = pl.ds(pl.multiple_of(i * step, step), step)
            part[r, :] = jnp.dot(at[r, :], eup[...], preferred_element_type=F32)
            return carry
        lax.fori_loop(0, items // step, mm2, 0)
        r12[me] = part[own_i, :]

        def send_rs(p):
            send(part.at[pl.ds(pl.multiple_of(p * shard, shard), shard)], r12.at[me], rs_s, rs_r, {"row": p})
        each_peer(send_rs)
        wait_bytes(r12.at[pl.ds(0, rows_n - 1)], rs_r)
        panel[own_i, :] = jnp.sum(r12[...], axis=0).astype(BF16)
        each_peer(lambda p: send(panel.at[own_i], panel.at[own_i], ag_s, ag_r, {"row": p}))
        wait_bytes(panel.at[pl.ds(0, (rows_n - 1) * shard)], ag_r)

        quarter = users // 4
        for k in range(4):
            r = slice(k * quarter, (k + 1) * quarter)
            up3[r, :] = jnp.dot(a[r, :], panel[...], preferred_element_type=F32)
            send(up3.at[pl.ds(k * quarter, quarter)], ur3.at[pl.ds(k * quarter, quarter)],
                 u3_s.at[k], u3_r.at[k], {"col": 1 - col})
        for k in range(4):
            r = slice(k * quarter, (k + 1) * quarter)
            wait_bytes(ur3.at[pl.ds(k * quarter, quarter)], u3_r.at[k])
            s = up3[r, :] + ur3[r, :]
            eu23[r, :] = s.astype(BF16)
            eud[r, :] = dup_lo(s).astype(BF16)

        groups = step // shard

        def mm4(i, carry):
            r = pl.ds(pl.multiple_of(i * step, step), step)
            v = jnp.dot(at[r, :], eud[...], preferred_element_type=F32).reshape(groups, shard, LANES)
            lo, hi = v[:, 0:shard // 2, :], v[:, shard // 2:shard, :]
            ln = lax.broadcasted_iota(jnp.int32, lo.shape, 2)
            p3[pl.ds(i * groups, groups)] = jnp.where(ln < 64, lo, hi)
            return carry
        lax.fori_loop(0, items // step, mm4, 0)
        r3[me] = p3[me]
        each_peer(lambda p: send(p3.at[p], r3.at[me], r3_s, r3_r, {"row": p}))

        for k in range(4):
            r = slice(k * quarter, (k + 1) * quarter)
            x = eup[r, :].astype(F32)
            y = eu23[r, :].astype(F32)
            t = x + pltpu.roll(x, 64, 1)
            outd[r, :] = ((t + dup_lo(y) + dup_hi(y)) * 0.25).astype(BF16)
        outu[...] = outd[own_u, 0:64]
        c_ou = pltpu.make_async_copy(outu, ou_hbm, out_sem.at[0])
        c_ou.start()
        trips = trip[...]
        ids = lax.broadcasted_iota(jnp.int32, (trips.shape[0], users), 1) + me * users
        hot = jnp.where(ids == trips[:, 0:1], 1.0, 0.0).astype(BF16)
        picked = jnp.dot(hot, outd[...], preferred_element_type=F32)
        tq = picked.shape[0] // 2
        ln = lax.broadcasted_iota(jnp.int32, (tq, LANES), 1)
        ea[...] = jnp.where(ln < 64, picked[0:tq], picked[tq:2 * tq]).astype(BF16)
        for o in range(1, side):
            send(ea, ear1.at[o - 1], ea1_s.at[o - 1], ea1_r.at[o - 1],
                 {"row": (mx + o) % side + side * my + plane * mz})
        for o in range(1, side):
            wait_bytes(ear1.at[o - 1], ea1_r.at[o - 1])
        ea1[...] = (ea[...].astype(F32) + jnp.sum(ear1[...].astype(F32), axis=0)).astype(BF16)

        def send_ea(o, carry):
            pyz = side * ((my + o % side) % side) + plane * ((mz + o // side) % side)
            send(ea1, ear2.at[o], ea2_s, ea2_r, {"row": mx + pyz})
            return carry
        lax.fori_loop(1, plane, send_ea, 0)
        ear2[0] = ea1[...]
        wait_bytes(ear2.at[pl.ds(0, plane - 1)], ea2_r)
        eav = jnp.sum(ear2[...].astype(F32), axis=0)
        users_v = jnp.concatenate([eav[:, 0:64], pltpu.roll(eav, 64, 1)[:, 0:64]], axis=0).astype(BF16)
        pad = jnp.concatenate([trips, jnp.zeros((trips.shape[0], LANES - 3), jnp.int32)], axis=1).astype(F32)
        tr = jnp.transpose(pad)
        base = (col * items + me * shard).astype(F32)
        rowid = lax.broadcasted_iota(jnp.int32, (shard, LANES), 0).astype(F32) + base
        g = panel[own_i, :].astype(F32)
        e0own = e0d[own_i, :].astype(F32)
        tot = e0own + dup_lo(g) + dup_hi(g)

        wait_bytes(r3.at[pl.ds(0, rows_n - 1)], r3_r)
        s3 = jnp.sum(r3[...], axis=0).astype(BF16).astype(F32)
        e3 = jnp.concatenate([dup_lo(s3), dup_hi(s3)], axis=0)
        oi = ((tot + e3) * 0.25).astype(BF16)
        outi[...] = oi[:, 0:64]
        c_oi = pltpu.make_async_copy(outi, oi_hbm, out_sem.at[1])
        c_oi.start()

        dots = lax.dot_general(oi[:, 0:64], users_v, (((1,), (1,)), ((), ())), preferred_element_type=F32)
        xp = jnp.sum(jnp.where(rowid == tr[1:2, :], dots, 0.0), axis=0, keepdims=True)
        xn = jnp.sum(jnp.where(rowid == tr[2:3, :], dots, 0.0), axis=0, keepdims=True)
        xs[me, 0:1, :] = xp - xn
        line = pl.ds(0, 1)
        each_peer(lambda p: send(xs.at[me, line], xs.at[me, line], xs_s, xs_r, {"row": p}))
        wait_bytes(xs.at[pl.ds(0, rows_n - 1), line], xs_r)
        xd[col, 0:1, :] = jnp.sum(xs[:, 0:1, :], axis=0)
        send(xd.at[col, line], xd.at[col, line], xd_s, xd_r, {"col": 1 - col})
        wait_bytes(xd.at[0, line], xd_r)
        neg = -(xd[0, 0:1, :] + xd[1, 0:1, :])
        sp = jnp.maximum(neg, 0.0) + jnp.log1p(jnp.exp(-jnp.abs(neg)))
        lossv[...] = jnp.sum(sp, axis=1, keepdims=True) * (1.0 / sp.shape[1])
        c_lo = pltpu.make_async_copy(lossv, loss_hbm, out_sem.at[2])
        c_lo.start()

        wait_bytes(deg.at[pl.ds(0, rows_n - 1)], deg_s)
        wait_bytes(e0.at[pl.ds(0, (rows_n - 1) * shard)], e0_s)
        wait_bytes(eu0.at[pl.ds(0, half)], eu0_s)
        wait_bytes(usum.at[0], us_s)
        wait_bytes(up1, u1_s)
        wait_bytes(r12.at[pl.ds(0, rows_n - 1)], rs_s)
        wait_bytes(panel.at[pl.ds(0, (rows_n - 1) * shard)], ag_s)
        for k in range(4):
            wait_bytes(up3.at[pl.ds(k * quarter, quarter)], u3_s.at[k])
        wait_bytes(p3.at[pl.ds(0, rows_n - 1)], r3_s)
        for o in range(1, side):
            wait_bytes(ea, ea1_s.at[o - 1])
        wait_bytes(ear2.at[pl.ds(0, plane - 1)], ea2_s)
        wait_bytes(xs.at[pl.ds(0, rows_n - 1), line], xs_s)
        wait_bytes(xd.at[0, line], xd_s)
        c_ou.wait()
        c_oi.wait()
        c_lo.wait()

    def local_prog(mask_blk, user_shard, item_shard, triples):
        users, items = mask_blk.shape
        half, dim = user_shard.shape
        shard = item_shard.shape[0]
        trips = triples.shape[0]
        V = pltpu.VMEM
        D = pltpu.SemaphoreType.DMA
        scratch = [
            V((users, items), jnp.int32), V((users, items), BF16), V((items, users), BF16),
            V((8, items), F32), V((trips, 3), jnp.int32),
            V((rows_n, items // LANES, LANES), F32), V((2, users // LANES, LANES), F32),
            V((users, LANES), F32), V((items // LANES, LANES), F32), V((items, LANES), F32),
            V((items, dim), BF16), V((items, LANES), BF16), V((users, LANES), BF16), V((users, dim), BF16),
            V((half, LANES), F32), V((half, LANES), F32),
            V((items, LANES), F32), V((rows_n, shard, LANES), F32), V((items, LANES), BF16),
            V((users, LANES), F32), V((users, LANES), F32), V((users, LANES), BF16), V((users, LANES), BF16),
            V((rows_n, shard // 2, LANES), F32), V((rows_n, shard // 2, LANES), F32),
            V((users, LANES), BF16), V((half, dim), BF16), V((shard, dim), BF16),
            V((trips // 2, LANES), BF16), V((side - 1, trips // 2, LANES), BF16),
            V((trips // 2, LANES), BF16), V((plane, trips // 2, LANES), BF16),
            V((rows_n, 8, LANES), F32), V((2, 8, LANES), F32), V((1, 1), F32),
            D((users // LANES,)), D((3,)), D((3,)),
        ] + [D, D] * 7
        scratch += [D((4,)), D((4,)), D, D, D((side - 1,)), D((side - 1,)), D, D, D, D, D, D]
        ANY = pl.BlockSpec(memory_space=pl.ANY)
        out_user, out_item, loss = pl.pallas_call(
            kernel,
            out_shape=(jax.ShapeDtypeStruct((half, dim), BF16), jax.ShapeDtypeStruct((shard, dim), BF16),
                       jax.ShapeDtypeStruct((1, 1), F32)),
            in_specs=[ANY] * 4,
            out_specs=(ANY,) * 3,
            scratch_shapes=scratch,
            compiler_params=pltpu.CompilerParams(collective_id=0, has_side_effects=True,
                                                 vmem_limit_bytes=56 << 20),
        )(mask_blk, user_shard, item_shard, triples)
        return out_user, out_item, loss[0, 0]

    return jax.shard_map(local_prog, mesh=mesh, in_specs=(P("row", "col"), P(("row", "col"), None), P(("col", "row"), None), P(None, None)), out_specs=(P(("row", "col"), None), P(("col", "row"), None), P()), check_vma=False)
```

```python
import jax
import jax.numpy as jnp
from jax import lax
from jax.experimental import pallas as pl
from jax.experimental.pallas import tpu as pltpu
from jax.sharding import PartitionSpec as P

F32 = jnp.float32
BF16 = jnp.bfloat16
LANES = 128
DIM = 64


def solution(mesh):
    rows_n = mesh.shape["row"]
    side = round(rows_n ** (1 / 3))
    plane = side * side

    def far(d):
        return min(d, side - d)

    offsets = [(dx, dy, dz) for dz in range(side) for dy in range(side) for dx in range(side)]
    offsets = sorted(offsets[1:], key=lambda o: -(far(o[0]) + far(o[1]) + far(o[2])))

    def kernel(m_hbm, eu_hbm, ei_hbm, trip_hbm, ou_hbm, oi_hbm, loss_hbm,
               m32, a, at, cacc, trip, deg, usum, suc, svr, eu0t, ei0, e0p, eu0d, e0d, pan1, pan2,
               up1, ur1, up2, ur2, up3, ur3, eu1d, eu2d, eu3d, q1, q2, q3, r1, r2, r3, g1, g2, outd, outu, outi,
               ea, ear1, ea1, ear2, xs, xd, lossv,
               m_sem, in_sem, out_sem,
               deg_s, deg_r, e0_s, e0_r, eu0_s, eu0_r, us_s, us_r, u1_s, u1_r, u2_s, u2_r, u3_s, u3_r,
               r1_s, r1_r, r2_s, r2_r, r3_s, r3_r, g1_s, g1_r, g2_s, g2_r,
               ea1_s, ea1_r, ea2_s, ea2_r, xs_s, xs_r, xd_s, xd_r):
        me = lax.axis_index("row")
        col = lax.axis_index("col")
        mx = me % side
        my = (me // side) % side
        mz = me // plane
        pxs = [(mx + d) % side for d in range(side)]
        pys = [((my + d) % side) * side for d in range(side)]
        pzs = [((mz + d) % side) * plane for d in range(side)]
        users, items = a.shape
        half = users // 2
        shard = items // rows_n
        hs = shard // 2
        ublk = users // LANES
        iblk = items // LANES
        others = pl.ds(0, rows_n - 1)
        line = pl.ds(0, 1)

        def peer(o):
            return pxs[o[0]] + pys[o[1]] + pzs[o[2]]

        def lo_lanes(v):
            return lax.broadcasted_iota(jnp.int32, v.shape, v.ndim - 1) < DIM

        def dup_lo(v):
            return jnp.where(lo_lanes(v), v, pltpu.roll(v, DIM, v.ndim - 1))

        def dup_hi(v):
            return jnp.where(lo_lanes(v), pltpu.roll(v, DIM, v.ndim - 1), v)

        def send(src, dst, ssem, rsem, where):
            pltpu.make_async_remote_copy(src_ref=src, dst_ref=dst, send_sem=ssem, recv_sem=rsem,
                                         device_id=where).start()

        def wait_bytes(ref, sem):
            pltpu.make_async_copy(ref, ref, sem).wait()

        def spread(ref, ssem, rsem):
            for o in offsets:
                send(ref, ref, ssem, rsem, {"row": peer(o)})

        def unpack(src, dst):
            def body(i, carry):
                v = src[pl.ds(i * plane, plane)].astype(F32)
                both = jnp.concatenate([dup_lo(v), dup_hi(v)], axis=1).astype(BF16)
                dst[pl.ds(pl.multiple_of(i * plane * shard, plane * shard), plane * shard), :] = both.reshape(plane * shard, LANES)
                return carry
            lax.fori_loop(0, rows_n // plane, body, 0)

        m_copies = []
        for b in range(ublk):
            blk = pl.ds(b * LANES, LANES)
            m_copies.append(pltpu.make_async_copy(m_hbm.at[blk], m32.at[blk], m_sem.at[b]))
            m_copies[-1].start()
        c_eu = pltpu.make_async_copy(eu_hbm, eu0t.at[col], in_sem.at[0])
        c_ei = pltpu.make_async_copy(ei_hbm, ei0, in_sem.at[1])
        c_tr = pltpu.make_async_copy(trip_hbm, trip, in_sem.at[2])
        c_eu.start()
        c_ei.start()
        c_tr.start()
        barrier = pltpu.get_barrier_semaphore()
        for o in offsets:
            pl.semaphore_signal(barrier, inc=1, device_id={"row": peer(o)})
        pl.semaphore_signal(barrier, inc=1, device_id={"col": 1 - col})

        cacc[...] = jnp.zeros_like(cacc)
        for b in range(ublk):
            m_copies[b].wait()

            def colsum(i, carry):
                r = pl.ds(pl.multiple_of(b * LANES + i * 32, 32), 32)
                v = m32[r, :].astype(F32)
                cacc[...] += jnp.sum(v.reshape(4, 8, items), axis=0)
                a[r, :] = v.astype(BF16)
                return carry
            lax.fori_loop(0, LANES // 32, colsum, 0)
        dsum = jnp.sum(cacc[...], axis=0, keepdims=True)
        for i in range(iblk):
            deg[me, i:i + 1, :] = dsum[:, i * LANES:(i + 1) * LANES]
        c_eu.wait()
        c_ei.wait()
        c_tr.wait()
        own0 = jnp.concatenate([ei0[...], ei0[...]], axis=1).astype(F32)
        e0p[me] = jnp.where(lo_lanes(own0[0:hs]), own0[0:hs], own0[hs:shard]).astype(BF16)
        pl.semaphore_wait(barrier, rows_n)
        spread(deg.at[me], deg_s, deg_r)
        send(eu0t.at[col], eu0t.at[col], eu0_s, eu0_r, {"col": 1 - col})

        ones = jnp.ones((items, LANES), BF16)
        for b in range(ublk):
            rsum = jnp.dot(a[b * LANES:(b + 1) * LANES, :], ones, preferred_element_type=F32)
            usum[col, b:b + 1, :] = jnp.transpose(rsum)[0:1, :]
        send(usum.at[col], usum.at[col], us_s, us_r, {"col": 1 - col})
        spread(e0p.at[me], e0_s, e0_r)

        def flip(i, carry):
            c = pl.ds(pl.multiple_of(i * LANES, LANES), LANES)
            at[c, :] = jnp.transpose(a[:, c])
            return carry
        lax.fori_loop(0, iblk, flip, 0)
        wait_bytes(usum.at[0], us_r)
        su = lax.rsqrt(jnp.maximum(usum[0] + usum[1], 1.0))
        for b in range(ublk):
            suc[b * LANES:(b + 1) * LANES, :] = jnp.transpose(jnp.broadcast_to(su[b:b + 1, :], (LANES, LANES)))
        wait_bytes(eu0t.at[0], eu0_r)
        for c in range(2):
            t = eu0t[c]
            eu0d[c * half:(c + 1) * half, :] = jnp.transpose(jnp.concatenate([t, t], axis=0))

        wait_bytes(deg.at[others], deg_r)
        svr[...] = lax.rsqrt(jnp.maximum(jnp.sum(deg[...], axis=0), 1.0))

        def scale_at(i, carry):
            r = pl.ds(pl.multiple_of(i * LANES, LANES), LANES)
            sv = jnp.transpose(jnp.broadcast_to(svr[pl.ds(i, 1), :], (LANES, LANES)))
            for b in range(ublk):
                c = slice(b * LANES, (b + 1) * LANES)
                at[r, c] = at[r, c] * (su[b:b + 1, :] * sv).astype(BF16)
            return carry
        lax.fori_loop(0, iblk, scale_at, 0)

        def item_sums(eud, q, r, ssem, rsem):
            step = plane * shard
            for dz in sorted(range(side), key=lambda d: -far(d)):
                z = pzs[dz]
                rows = pl.ds(pl.multiple_of(z * shard, step), step)
                v = jnp.dot(at[rows, :], eud[...], preferred_element_type=F32).reshape(plane, shard, LANES)
                lo, hi = v[:, 0:hs, :], v[:, hs:shard, :]
                q[pl.ds(z, plane)] = jnp.where(lo_lanes(lo), lo, hi)
                for o in offsets:
                    if o[2] == dz:
                        p = peer(o)
                        send(q.at[p], r.at[me], ssem, rsem, {"row": p})
            r[me] = q[me]

        def user_sums(pan, up, ur, ssem, rsem):
            h = half // 2
            for k in range(2):
                lo = jnp.dot(a[k * h:(k + 1) * h, :], pan[...], preferred_element_type=F32)
                hi = jnp.dot(a[half + k * h:half + (k + 1) * h, :], pan[...], preferred_element_type=F32)
                up[k * h:(k + 1) * h, :] = jnp.where(lo_lanes(lo), lo, hi)
                send(up.at[pl.ds(k * h, h)], ur.at[pl.ds(k * h, h)], ssem.at[k], rsem.at[k], {"col": 1 - col})

        def user_rows(up, ur, rsem, eud):
            h = half // 2
            for k in range(2):
                wait_bytes(ur.at[pl.ds(k * h, h)], rsem.at[k])
                s = up[k * h:(k + 1) * h, :] + ur[k * h:(k + 1) * h, :]
                eud[k * h:(k + 1) * h, :] = dup_lo(s).astype(BF16)
                eud[half + k * h:half + (k + 1) * h, :] = dup_hi(s).astype(BF16)

        item_sums(eu0d, q1, r1, r1_s, r1_r)

        def scale_a(i, carry):
            c = pl.ds(pl.multiple_of(i * LANES, LANES), LANES)
            a[:, c] = a[:, c] * (suc[...] * svr[pl.ds(i, 1), :]).astype(BF16)
            return carry
        lax.fori_loop(0, iblk, scale_a, 0)
        wait_bytes(e0p.at[others], e0_r)
        unpack(e0p, e0d)
        user_sums(e0d, up1, ur1, u1_s, u1_r)
        user_rows(up1, ur1, u1_r, eu1d)
        item_sums(eu1d, q2, r2, r2_s, r2_r)
        wait_bytes(r1.at[others], r1_r)
        g1[me] = jnp.sum(r1[...], axis=0).astype(BF16)
        spread(g1.at[me], g1_s, g1_r)
        wait_bytes(r2.at[others], r2_r)
        g2[me] = jnp.sum(r2[...], axis=0).astype(BF16)
        spread(g2.at[me], g2_s, g2_r)
        wait_bytes(g1.at[others], g1_r)
        unpack(g1, pan1)
        user_sums(pan1, up2, ur2, u2_s, u2_r)
        user_rows(up2, ur2, u2_r, eu2d)
        item_sums(eu2d, q3, r3, r3_s, r3_r)
        wait_bytes(g2.at[others], g2_r)
        unpack(g2, pan2)
        user_sums(pan2, up3, ur3, u3_s, u3_r)
        user_rows(up3, ur3, u3_r, eu3d)

        quarter = users // 4
        for k in range(4):
            r = slice(k * quarter, (k + 1) * quarter)
            t = eu0d[r, :].astype(F32) + eu1d[r, :].astype(F32) + eu2d[r, :].astype(F32) + eu3d[r, :].astype(F32)
            outd[r, :] = (t * 0.25).astype(BF16)
        trips = trip[...]
        tn = trips.shape[1]
        ids = lax.broadcasted_iota(jnp.int32, (users, tn), 0) + me * users
        hot = jnp.where(ids == trips[0:1, :], 1.0, 0.0)
        picked = jnp.dot(jnp.transpose(hot).astype(BF16), outd[...], preferred_element_type=F32)
        tq = tn // 2
        ea[...] = jnp.where(lo_lanes(picked[0:tq]), picked[0:tq], picked[tq:tn]).astype(BF16)
        for o in (2, 1, 3):
            send(ea, ear1.at[o - 1], ea1_s.at[o - 1], ea1_r.at[o - 1], {"row": pxs[o] + pys[0] + pzs[0]})
        outu[...] = jnp.transpose(outd[pl.ds(pl.multiple_of(col * half, half), half), :])[0:DIM, :]
        c_ou = pltpu.make_async_copy(outu, ou_hbm, out_sem.at[0])
        c_ou.start()
        for o in range(1, side):
            wait_bytes(ear1.at[o - 1], ea1_r.at[o - 1])
        ea1[...] = (ea[...].astype(F32) + jnp.sum(ear1[...].astype(F32), axis=0)).astype(BF16)
        for o in offsets:
            if o[0] == 0:
                send(ea1, ear2.at[o[1] + side * o[2]], ea2_s, ea2_r, {"row": peer(o)})
        ear2[0] = ea1[...]
        g = g1[me].astype(F32)
        h = g2[me].astype(F32)
        tot = (own0 + jnp.concatenate([dup_lo(g), dup_hi(g)], axis=0)) + jnp.concatenate([dup_lo(h), dup_hi(h)], axis=0)
        rowid = lax.broadcasted_iota(jnp.int32, (shard, LANES), 0) + (col * items + me * shard)
        wait_bytes(r3.at[others], r3_r)
        s3 = jnp.sum(r3[...], axis=0).astype(BF16).astype(F32)
        oi = ((tot + jnp.concatenate([dup_lo(s3), dup_hi(s3)], axis=0)) * 0.25).astype(BF16)
        outi[...] = oi[:, 0:DIM]
        c_oi = pltpu.make_async_copy(outi, oi_hbm, out_sem.at[1])
        c_oi.start()
        wait_bytes(ear2.at[pl.ds(0, plane - 1)], ea2_r)
        eav = jnp.sum(ear2[...].astype(F32), axis=0)
        users_v = jnp.concatenate([eav[:, 0:DIM], pltpu.roll(eav, DIM, 1)[:, 0:DIM]], axis=0).astype(BF16)

        dots = lax.dot_general(oi[:, 0:DIM], users_v, (((1,), (1,)), ((), ())), preferred_element_type=F32)
        xp = jnp.sum(jnp.where(rowid == trips[1:2, :], dots, 0.0), axis=0, keepdims=True)
        xn = jnp.sum(jnp.where(rowid == trips[2:3, :], dots, 0.0), axis=0, keepdims=True)
        xs[me, 0:1, :] = xp - xn
        spread(xs.at[me, line], xs_s, xs_r)
        wait_bytes(xs.at[others, line], xs_r)
        xd[col, 0:1, :] = jnp.sum(xs[:, 0:1, :], axis=0)
        send(xd.at[col, line], xd.at[col, line], xd_s, xd_r, {"col": 1 - col})
        wait_bytes(xd.at[0, line], xd_r)
        neg = -(xd[0, 0:1, :] + xd[1, 0:1, :])
        sp = jnp.maximum(neg, 0.0) + jnp.log1p(jnp.exp(-jnp.abs(neg)))
        lossv[...] = jnp.sum(sp, axis=1, keepdims=True) * (1.0 / sp.shape[1])
        c_lo = pltpu.make_async_copy(lossv, loss_hbm, out_sem.at[2])
        c_lo.start()

        wait_bytes(deg.at[others], deg_s)
        wait_bytes(e0p.at[others], e0_s)
        wait_bytes(eu0t.at[0], eu0_s)
        wait_bytes(usum.at[0], us_s)
        for up, sem in ((up1, u1_s), (up2, u2_s), (up3, u3_s)):
            for k in range(2):
                wait_bytes(up.at[pl.ds(0, half // 2)], sem.at[k])
        wait_bytes(r1.at[others], r1_s)
        wait_bytes(r2.at[others], r2_s)
        wait_bytes(r3.at[others], r3_s)
        wait_bytes(g1.at[others], g1_s)
        wait_bytes(g2.at[others], g2_s)
        for o in range(1, side):
            wait_bytes(ea, ea1_s.at[o - 1])
        wait_bytes(ear2.at[pl.ds(0, plane - 1)], ea2_s)
        wait_bytes(xs.at[others, line], xs_s)
        wait_bytes(xd.at[0, line], xd_s)
        c_ou.wait()
        c_oi.wait()
        c_lo.wait()

    def local_prog(mask_blk, user_shard, item_shard, triples):
        users, items = mask_blk.shape
        half, dim = user_shard.shape
        shard = item_shard.shape[0]
        trips = triples.shape[0]
        V = pltpu.VMEM
        D = pltpu.SemaphoreType.DMA
        packed = (rows_n, shard // 2, LANES)
        scratch = [
            V((users, items), jnp.int32), V((users, items), BF16), V((items, users), BF16),
            V((8, items), F32), V((3, trips), jnp.int32),
            V((rows_n, items // LANES, LANES), F32), V((2, users // LANES, LANES), F32),
            V((users, LANES), F32), V((items // LANES, LANES), F32),
            V((2, dim, half), BF16), V((shard, dim), BF16), V(packed, BF16),
            V((users, LANES), BF16), V((items, LANES), BF16), V((items, LANES), BF16), V((items, LANES), BF16),
        ] + [V((half, LANES), F32)] * 6 + [V((users, LANES), BF16)] * 3 + [V(packed, F32)] * 6 + [V(packed, BF16)] * 2 + [
            V((users, LANES), BF16), V((dim, half), BF16), V((shard, dim), BF16),
            V((trips // 2, LANES), BF16), V((side - 1, trips // 2, LANES), BF16),
            V((trips // 2, LANES), BF16), V((plane, trips // 2, LANES), BF16),
            V((rows_n, 8, LANES), F32), V((2, 8, LANES), F32), V((1, 1), F32),
            D((users // LANES,)), D((3,)), D((3,)),
        ] + [D] * 8 + [D((2,))] * 6 + [D] * 10 + [D((side - 1,))] * 2 + [D] * 6
        ANY = pl.BlockSpec(memory_space=pl.ANY)
        out_user, out_item, loss = pl.pallas_call(
            kernel,
            out_shape=(jax.ShapeDtypeStruct((dim, half), BF16), jax.ShapeDtypeStruct((shard, dim), BF16),
                       jax.ShapeDtypeStruct((1, 1), F32)),
            in_specs=[ANY] * 4,
            out_specs=(ANY,) * 3,
            scratch_shapes=scratch,
            compiler_params=pltpu.CompilerParams(collective_id=0, has_side_effects=True,
                                                 vmem_limit_bytes=56 << 20),
        )(mask_blk, user_shard.T, item_shard, triples.T)
        return out_user.T, out_item, loss[0, 0]

    return jax.shard_map(local_prog, mesh=mesh, in_specs=(P("row", "col"), P(("row", "col"), None), P(("col", "row"), None), P(None, None)), out_specs=(P(("row", "col"), None), P(("col", "row"), None), P()), check_vma=False)
```

```python
import jax
import jax.numpy as jnp
from jax import lax
from jax.experimental import pallas as pl
from jax.experimental.pallas import tpu as pltpu
from jax.sharding import PartitionSpec as P

F32 = jnp.float32
BF16 = jnp.bfloat16
LANES = 128
DIM = 64


def solution(mesh):
    rows_n = mesh.shape["row"]
    side = round(rows_n ** (1 / 3))
    plane = side * side

    def far(d):
        return min(d, side - d)

    offsets = [(dx, dy, dz) for dz in range(side) for dy in range(side) for dx in range(side)]
    offsets = sorted(offsets[1:], key=lambda o: -(far(o[0]) + far(o[1]) + far(o[2])))

    def kernel(m_hbm, eu_hbm, ei_hbm, trip_hbm, ou_hbm, oi_hbm, loss_hbm,
               m32, a, at, cacc, trip, deg, usum, suc, svr, svc, eu0t, ei0, e0p, e0d, pan1, pan2,
               up1, ur1, up2, ur2, up3, ur3, w0, w1, w2, eu0, eu1, eu2, eu3, q1, q2, q3, r1, r2, r3, g1, g2, outp, outu, outi,
               ea, ear1, ea1, ear2, xs, lossv,
               m_sem, in_sem, out_sem,
               deg_s, deg_r, e0_s, e0_r, eu0_s, eu0_r, us_s, us_r, u1_s, u1_r, u2_s, u2_r, u3_s, u3_r,
               r1_s, r1_r, r2_s, r2_r, r3_s, r3_r, g1_s, g1_r, g2_s, g2_r,
               ea1_s, ea1_r, ea2_s, ea2_r, xs_s, xs_r):
        me = lax.axis_index("row")
        col = lax.axis_index("col")
        mx = me % side
        my = (me // side) % side
        mz = me // plane
        pxs = [(mx + d) % side for d in range(side)]
        pys = [((my + d) % side) * side for d in range(side)]
        pzs = [((mz + d) % side) * plane for d in range(side)]
        users, items = a.shape
        half = users // 2
        shard = items // rows_n
        hs = shard // 2
        ublk = users // LANES
        iblk = items // LANES
        others = pl.ds(0, rows_n - 1)
        line = pl.ds(0, 1)

        def peer(o):
            return pxs[o[0]] + pys[o[1]] + pzs[o[2]]

        def lo_lanes(v):
            return lax.broadcasted_iota(jnp.int32, v.shape, v.ndim - 1) < DIM

        def dup_lo(v):
            return jnp.where(lo_lanes(v), v, pltpu.roll(v, DIM, v.ndim - 1))

        def dup_hi(v):
            return jnp.where(lo_lanes(v), pltpu.roll(v, DIM, v.ndim - 1), v)

        def send(src, dst, ssem, rsem, where):
            pltpu.make_async_remote_copy(src_ref=src, dst_ref=dst, send_sem=ssem, recv_sem=rsem,
                                         device_id=where).start()

        def wait_bytes(ref, sem):
            pltpu.make_async_copy(ref, ref, sem).wait()

        def spread(ref, ssem, rsem):
            for o in offsets:
                send(ref, ref, ssem, rsem, {"row": peer(o)})

        def unpack(src, dst):
            def body(i, carry):
                v = src[pl.ds(i * plane, plane)].astype(F32)
                both = jnp.concatenate([dup_lo(v), dup_hi(v)], axis=1).astype(BF16)
                dst[pl.ds(pl.multiple_of(i * plane * shard, plane * shard), plane * shard), :] = both.reshape(plane * shard, LANES)
                return carry
            lax.fori_loop(0, rows_n // plane, body, 0)

        def stack(v, w, k):
            n = v.shape[0]
            t = pltpu.roll(v, DIM, 1)
            lo = lo_lanes(v)
            for i, x in enumerate((jnp.where(lo, v, 0.0), jnp.where(lo, t, 0.0), jnp.where(lo, 0.0, t), jnp.where(lo, 0.0, v))):
                w[i * half + k * n:i * half + (k + 1) * n, :] = x.astype(BF16)

        m_copies = []
        for b in range(ublk):
            blk = pl.ds(b * LANES, LANES)
            m_copies.append(pltpu.make_async_copy(m_hbm.at[blk], m32.at[blk], m_sem.at[b]))
            m_copies[-1].start()
        c_eu = pltpu.make_async_copy(eu_hbm, eu0t.at[col], in_sem.at[0])
        c_ei = pltpu.make_async_copy(ei_hbm, ei0, in_sem.at[1])
        c_tr = pltpu.make_async_copy(trip_hbm, trip, in_sem.at[2])
        c_eu.start()
        c_ei.start()
        c_tr.start()
        barrier = pltpu.get_barrier_semaphore()
        for o in offsets:
            pl.semaphore_signal(barrier, inc=1, device_id={"row": peer(o)})
            pl.semaphore_signal(barrier, inc=1, device_id={"row": peer(o), "col": 1 - col})
        pl.semaphore_signal(barrier, inc=1, device_id={"col": 1 - col})

        cacc[...] = jnp.zeros_like(cacc)
        for b in range(ublk):
            m_copies[b].wait()

            def colsum(i, carry):
                r = pl.ds(pl.multiple_of(b * LANES + i * 32, 32), 32)
                v = m32[r, :].astype(F32)
                cacc[...] += jnp.sum(v.reshape(4, 8, items), axis=0)
                a[r, :] = v.astype(BF16)
                return carry
            lax.fori_loop(0, LANES // 32, colsum, 0)
        dsum = jnp.sum(cacc[...], axis=0, keepdims=True)
        for i in range(iblk):
            deg[me, i:i + 1, :] = dsum[:, i * LANES:(i + 1) * LANES]
        c_eu.wait()
        c_ei.wait()
        c_tr.wait()
        own0 = jnp.concatenate([ei0[...], ei0[...]], axis=1).astype(F32)
        e0p[me] = jnp.where(lo_lanes(own0[0:hs]), own0[0:hs], own0[hs:shard]).astype(BF16)
        pl.semaphore_wait(barrier, 2 * rows_n - 1)
        spread(deg.at[me], deg_s, deg_r)
        send(eu0t.at[col], eu0t.at[col], eu0_s, eu0_r, {"col": 1 - col})

        ones = jnp.ones((items, LANES), BF16)
        for b in range(ublk):
            rsum = jnp.dot(a[b * LANES:(b + 1) * LANES, :], ones, preferred_element_type=F32)
            usum[col, b:b + 1, :] = jnp.transpose(rsum)[0:1, :]
        send(usum.at[col], usum.at[col], us_s, us_r, {"col": 1 - col})
        spread(e0p.at[me], e0_s, e0_r)

        def flip(i, carry):
            c = pl.ds(pl.multiple_of(i * LANES, LANES), LANES)
            t = jnp.transpose(a[:, c]).reshape(LANES // shard, 2, hs, users)
            r = pl.ds(pl.multiple_of(i * LANES // 2, LANES // 2), LANES // 2)
            at[r, 0:users] = t[:, 0].reshape(LANES // 2, users)
            at[r, users:2 * users] = t[:, 1].reshape(LANES // 2, users)
            return carry
        lax.fori_loop(0, iblk, flip, 0)
        wait_bytes(usum.at[0], us_r)
        su = lax.rsqrt(jnp.maximum(usum[0] + usum[1], 1.0))
        for b in range(ublk):
            suc[b * LANES:(b + 1) * LANES, :] = jnp.transpose(jnp.broadcast_to(su[b:b + 1, :], (LANES, LANES)))
        wait_bytes(eu0t.at[0], eu0_r)
        eu0[...] = jnp.transpose(jnp.concatenate([eu0t[0], eu0t[1]], axis=0))
        stack(eu0[...].astype(F32), w0, 0)

        wait_bytes(deg.at[others], deg_r)
        sv = lax.rsqrt(jnp.maximum(jnp.sum(deg[...], axis=0), 1.0))
        svr[...] = sv
        svt = jnp.transpose(jnp.concatenate([sv, jnp.zeros((LANES - iblk, LANES), F32)], axis=0))
        for i in range(iblk):
            t = jnp.broadcast_to(svt[:, i:i + 1], (LANES, LANES)).reshape(LANES // shard, 2, hs, LANES)
            for k in range(2):
                svc[k, i * LANES // 2:(i + 1) * LANES // 2, :] = t[:, k].reshape(LANES // 2, LANES)

        def scale_at(i, carry):
            r = pl.ds(pl.multiple_of(i * LANES, LANES), LANES)
            for k in range(2):
                t = svc[k, r, :]
                for b in range(ublk):
                    c = slice(k * users + b * LANES, k * users + (b + 1) * LANES)
                    at[r, c] = at[r, c] * (su[b:b + 1, :] * t).astype(BF16)
            return carry
        lax.fori_loop(0, items // 2 // LANES, scale_at, 0)

        def item_sums(w, q, r, ssem, rsem):
            step = plane * hs
            for dz in sorted(range(side), key=lambda d: -far(d)):
                z = pzs[dz]
                rows = pl.ds(pl.multiple_of(z * hs, step), step)
                v = jnp.dot(at[rows, :], w[...], preferred_element_type=F32)
                q[pl.ds(z, plane)] = v.reshape(plane, hs, LANES)
                for o in offsets:
                    if o[2] == dz:
                        p = peer(o)
                        send(q.at[p], r.at[me], ssem, rsem, {"row": p})
            r[me] = q[me]

        def user_sums(pan, up, ur, ssem, rsem):
            h = half // 2
            for k in range(2):
                lo = jnp.dot(a[k * h:(k + 1) * h, :], pan[...], preferred_element_type=F32)
                hi = jnp.dot(a[half + k * h:half + (k + 1) * h, :], pan[...], preferred_element_type=F32)
                up[k * h:(k + 1) * h, :] = jnp.where(lo_lanes(lo), lo, hi)
                send(up.at[pl.ds(k * h, h)], ur.at[pl.ds(k * h, h)], ssem.at[k], rsem.at[k], {"col": 1 - col})

        def user_rows(up, ur, rsem, eu, w):
            h = half // 2
            for k in range(2):
                wait_bytes(ur.at[pl.ds(k * h, h)], rsem.at[k])
                s = up[k * h:(k + 1) * h, :] + ur[k * h:(k + 1) * h, :]
                eu[k * h:(k + 1) * h, :] = s.astype(BF16)
                if w is not None:
                    stack(s, w, k)

        item_sums(w0, q1, r1, r1_s, r1_r)

        def scale_a(b, carry):
            r = pl.ds(pl.multiple_of(b * LANES, LANES), LANES)
            t = suc[r, :]
            for i in range(iblk):
                c = slice(i * LANES, (i + 1) * LANES)
                a[r, c] = a[r, c] * (t * svr[i:i + 1, :]).astype(BF16)
            return carry
        lax.fori_loop(0, ublk, scale_a, 0)
        wait_bytes(e0p.at[others], e0_r)
        unpack(e0p, e0d)
        user_sums(e0d, up1, ur1, u1_s, u1_r)
        user_rows(up1, ur1, u1_r, eu1, w1)
        item_sums(w1, q2, r2, r2_s, r2_r)
        wait_bytes(r1.at[others], r1_r)
        g1[me] = jnp.sum(r1[...], axis=0).astype(BF16)
        spread(g1.at[me], g1_s, g1_r)
        wait_bytes(r2.at[others], r2_r)
        g2[me] = jnp.sum(r2[...], axis=0).astype(BF16)
        spread(g2.at[me], g2_s, g2_r)
        wait_bytes(g1.at[others], g1_r)
        unpack(g1, pan1)
        user_sums(pan1, up2, ur2, u2_s, u2_r)
        user_rows(up2, ur2, u2_r, eu2, w2)
        item_sums(w2, q3, r3, r3_s, r3_r)
        wait_bytes(g2.at[others], g2_r)
        unpack(g2, pan2)
        user_sums(pan2, up3, ur3, u3_s, u3_r)
        user_rows(up3, ur3, u3_r, eu3, None)

        t = eu0[...].astype(F32) + eu1[...].astype(F32) + eu2[...].astype(F32) + eu3[...].astype(F32)
        outp[...] = (t * 0.25).astype(BF16)
        trips = trip[...]
        tn = trips.shape[1]
        tq = tn // 2
        ids = lax.broadcasted_iota(jnp.int32, (users, tn), 0) + me * users
        hot = jnp.transpose(jnp.where(ids == trips[0:1, :], 1.0, 0.0)).astype(BF16)
        first = jnp.dot(hot[:, 0:half], outp[...], preferred_element_type=F32)
        second = jnp.dot(hot[:, half:users], outp[...], preferred_element_type=F32)
        top = first[0:tq] + pltpu.roll(second[0:tq], DIM, 1)
        bot = pltpu.roll(first[tq:tn], DIM, 1) + second[tq:tn]
        ea[...] = jnp.where(lo_lanes(top), top, bot).astype(BF16)
        for o in (2, 1, 3):
            send(ea, ear1.at[o - 1], ea1_s.at[o - 1], ea1_r.at[o - 1], {"row": pxs[o] + pys[0] + pzs[0]})
        flat = jnp.transpose(outp[...])
        outu[...] = jnp.where(col == 0, flat[0:DIM, :], flat[DIM:2 * DIM, :])
        c_ou = pltpu.make_async_copy(outu, ou_hbm, out_sem.at[0])
        c_ou.start()
        for o in range(1, side):
            wait_bytes(ear1.at[o - 1], ea1_r.at[o - 1])
        ea1[...] = (ea[...].astype(F32) + jnp.sum(ear1[...].astype(F32), axis=0)).astype(BF16)
        for o in offsets:
            if o[0] == 0:
                send(ea1, ear2.at[o[1] + side * o[2]], ea2_s, ea2_r, {"row": peer(o)})
        ear2[0] = ea1[...]
        g = g1[me].astype(F32)
        h = g2[me].astype(F32)
        tot = (own0 + jnp.concatenate([dup_lo(g), dup_hi(g)], axis=0)) + jnp.concatenate([dup_lo(h), dup_hi(h)], axis=0)
        rowid = lax.broadcasted_iota(jnp.int32, (shard, LANES), 0) + (col * items + me * shard)
        wait_bytes(r3.at[others], r3_r)
        s3 = jnp.sum(r3[...], axis=0).astype(BF16).astype(F32)
        oi = ((tot + jnp.concatenate([dup_lo(s3), dup_hi(s3)], axis=0)) * 0.25).astype(BF16)
        outi[...] = oi[:, 0:DIM]
        c_oi = pltpu.make_async_copy(outi, oi_hbm, out_sem.at[1])
        c_oi.start()
        wait_bytes(ear2.at[pl.ds(0, plane - 1)], ea2_r)
        eav = jnp.sum(ear2[...].astype(F32), axis=0)
        users_v = jnp.concatenate([eav[:, 0:DIM], pltpu.roll(eav, DIM, 1)[:, 0:DIM]], axis=0).astype(BF16)

        dots = lax.dot_general(oi[:, 0:DIM], users_v, (((1,), (1,)), ((), ())), preferred_element_type=F32)
        xp = jnp.sum(jnp.where(rowid == trips[1:2, :], dots, 0.0), axis=0, keepdims=True)
        xn = jnp.sum(jnp.where(rowid == trips[2:3, :], dots, 0.0), axis=0, keepdims=True)
        mine = col * rows_n + me
        xs[mine, 0:1, :] = xp - xn
        for o in offsets:
            for c in (1 - col, col):
                send(xs.at[mine, line], xs.at[mine, line], xs_s, xs_r, {"row": peer(o), "col": c})
        send(xs.at[mine, line], xs.at[mine, line], xs_s, xs_r, {"col": 1 - col})
        wait_bytes(xs.at[pl.ds(0, 2 * rows_n - 1), line], xs_r)
        neg = -jnp.sum(xs[:, 0:1, :], axis=0)
        sp = jnp.maximum(neg, 0.0) + jnp.log1p(jnp.exp(-jnp.abs(neg)))
        lossv[...] = jnp.sum(sp, axis=1, keepdims=True) * (1.0 / sp.shape[1])
        c_lo = pltpu.make_async_copy(lossv, loss_hbm, out_sem.at[2])
        c_lo.start()

        wait_bytes(deg.at[others], deg_s)
        wait_bytes(e0p.at[others], e0_s)
        wait_bytes(eu0t.at[0], eu0_s)
        wait_bytes(usum.at[0], us_s)
        for up, sem in ((up1, u1_s), (up2, u2_s), (up3, u3_s)):
            for k in range(2):
                wait_bytes(up.at[pl.ds(0, half // 2)], sem.at[k])
        wait_bytes(r1.at[others], r1_s)
        wait_bytes(r2.at[others], r2_s)
        wait_bytes(r3.at[others], r3_s)
        wait_bytes(g1.at[others], g1_s)
        wait_bytes(g2.at[others], g2_s)
        for o in range(1, side):
            wait_bytes(ea, ea1_s.at[o - 1])
        wait_bytes(ear2.at[pl.ds(0, plane - 1)], ea2_s)
        wait_bytes(xs.at[pl.ds(0, 2 * rows_n - 1), line], xs_s)
        c_ou.wait()
        c_oi.wait()
        c_lo.wait()

    def local_prog(mask_blk, user_shard, item_shard, triples):
        users, items = mask_blk.shape
        half, dim = user_shard.shape
        shard = item_shard.shape[0]
        trips = triples.shape[0]
        V = pltpu.VMEM
        D = pltpu.SemaphoreType.DMA
        packed = (rows_n, shard // 2, LANES)
        scratch = [
            V((users, items), jnp.int32), V((users, items), BF16), V((items // 2, 2 * users), BF16),
            V((8, items), F32), V((3, trips), jnp.int32),
            V((rows_n, items // LANES, LANES), F32), V((2, users // LANES, LANES), F32),
            V((users, LANES), F32), V((items // LANES, LANES), F32), V((2, items // 2, LANES), F32),
            V((2, dim, half), BF16), V((shard, dim), BF16), V(packed, BF16),
        ] + [V((items, LANES), BF16)] * 3 + [V((half, LANES), F32)] * 6 + [V((2 * users, LANES), BF16)] * 3 + [
            V((half, LANES), BF16)] * 4 + [V(packed, F32)] * 6 + [V(packed, BF16)] * 2 + [
            V((half, LANES), BF16), V((dim, half), BF16), V((shard, dim), BF16),
            V((trips // 2, LANES), BF16), V((side - 1, trips // 2, LANES), BF16),
            V((trips // 2, LANES), BF16), V((plane, trips // 2, LANES), BF16),
            V((2 * rows_n, 8, LANES), F32), V((1, 1), F32),
            D((users // LANES,)), D((3,)), D((3,)),
        ] + [D] * 8 + [D((2,))] * 6 + [D] * 10 + [D((side - 1,))] * 2 + [D] * 4
        ANY = pl.BlockSpec(memory_space=pl.ANY)
        out_user, out_item, loss = pl.pallas_call(
            kernel,
            out_shape=(jax.ShapeDtypeStruct((dim, half), BF16), jax.ShapeDtypeStruct((shard, dim), BF16),
                       jax.ShapeDtypeStruct((1, 1), F32)),
            in_specs=[ANY] * 4,
            out_specs=(ANY,) * 3,
            scratch_shapes=scratch,
            compiler_params=pltpu.CompilerParams(collective_id=0, has_side_effects=True,
                                                 vmem_limit_bytes=56 << 20),
        )(mask_blk, user_shard.T, item_shard, triples.T)
        return out_user.T, out_item, loss[0, 0]

    return jax.shard_map(local_prog, mesh=mesh, in_specs=(P("row", "col"), P(("row", "col"), None), P(("col", "row"), None), P(None, None)), out_specs=(P(("row", "col"), None), P(("col", "row"), None), P()), check_vma=False)
```

```python
import jax
import jax.numpy as jnp
from jax import lax
from jax.experimental import pallas as pl
from jax.experimental.pallas import tpu as pltpu
from jax.sharding import PartitionSpec as P

F32 = jnp.float32
BF16 = jnp.bfloat16
LANES = 128
DIM = 64


def solution(mesh):
    rows_n = mesh.shape["row"]
    side = round(rows_n ** (1 / 3))
    plane = side * side

    def far(d):
        return min(d, side - d)

    offsets = [(dx, dy, dz) for dz in range(side) for dy in range(side) for dx in range(side)]
    offsets = sorted(offsets[1:], key=lambda o: -(far(o[0]) + far(o[1]) + far(o[2])))

    def kernel(m_hbm, eu_hbm, ei_hbm, trip_hbm, ou_hbm, oi_hbm, loss_hbm,
               m32, a, at, cacc, trip, deg, usum, suc, svr, svc, eu0t, ei0, e0p, e0d, pan1, pan2,
               up1, ur1, up2, ur2, up3, ur3, w0, w1, w2, eu0, eu1, eu2, eu3, q1, q2, q3, r1, r2, r3, g1, g2, outp, outu, outi,
               ea, ear1, ea1, ear2, xs, lossv, hot,
               m_sem, in_sem, out_sem,
               deg_s, deg_r, e0_s, e0_r, eu0_s, eu0_r, us_s, us_r, u1_s, u1_r, u2_s, u2_r, u3_s, u3_r,
               r1_s, r1_r, r2_s, r2_r, r3_s, r3_r, g1_s, g1_r, g2_s, g2_r,
               ea1_s, ea1_r, ea2_s, ea2_r, xs_s, xs_r):
        me = lax.axis_index("row")
        col = lax.axis_index("col")
        mx = me % side
        my = (me // side) % side
        mz = me // plane
        pxs = [(mx + d) % side for d in range(side)]
        pys = [((my + d) % side) * side for d in range(side)]
        pzs = [((mz + d) % side) * plane for d in range(side)]
        nxs = [(d - mx + side) % side for d in range(side)]
        nys = [((d - my + side) % side) * side for d in range(side)]
        users, items = a.shape
        half = users // 2
        shard = items // rows_n
        hs = shard // 2
        ublk = users // LANES
        iblk = items // LANES
        others = pl.ds(0, rows_n - 1)
        line = pl.ds(0, 1)

        def peer(o):
            return pxs[o[0]] + pys[o[1]] + pzs[o[2]]

        def lo_lanes(v):
            return lax.broadcasted_iota(jnp.int32, v.shape, v.ndim - 1) < DIM

        def dup_lo(v):
            return jnp.where(lo_lanes(v), v, pltpu.roll(v, DIM, v.ndim - 1))

        def dup_hi(v):
            return jnp.where(lo_lanes(v), pltpu.roll(v, DIM, v.ndim - 1), v)

        def send(src, dst, ssem, rsem, where):
            pltpu.make_async_remote_copy(src_ref=src, dst_ref=dst, send_sem=ssem, recv_sem=rsem,
                                         device_id=where).start()

        def wait_bytes(ref, sem):
            pltpu.make_async_copy(ref, ref, sem).wait()

        def spread(ref, ssem, rsem):
            for o in offsets:
                send(ref, ref, ssem, rsem, {"row": peer(o)})

        def unpack(src, dst):
            def body(i, carry):
                v = src[pl.ds(i * plane, plane)].astype(F32)
                both = jnp.concatenate([dup_lo(v), dup_hi(v)], axis=1).astype(BF16)
                dst[pl.ds(pl.multiple_of(i * plane * shard, plane * shard), plane * shard), :] = both.reshape(plane * shard, LANES)
                return carry
            lax.fori_loop(0, rows_n // plane, body, 0)

        def stack(v, w, k):
            n = v.shape[0]
            t = pltpu.roll(v, DIM, 1)
            lo = lo_lanes(v)
            for i, x in enumerate((jnp.where(lo, v, 0.0), jnp.where(lo, t, 0.0), jnp.where(lo, 0.0, t), jnp.where(lo, 0.0, v))):
                w[i * half + k * n:i * half + (k + 1) * n, :] = x.astype(BF16)

        m_copies = []
        for b in range(ublk):
            blk = pl.ds(b * LANES, LANES)
            m_copies.append(pltpu.make_async_copy(m_hbm.at[blk], m32.at[blk], m_sem.at[b]))
            m_copies[-1].start()
        c_eu = pltpu.make_async_copy(eu_hbm, eu0t.at[col], in_sem.at[0])
        c_ei = pltpu.make_async_copy(ei_hbm, ei0, in_sem.at[1])
        c_tr = pltpu.make_async_copy(trip_hbm, trip, in_sem.at[2])
        c_eu.start()
        c_ei.start()
        c_tr.start()
        barrier = pltpu.get_barrier_semaphore()
        for o in offsets:
            pl.semaphore_signal(barrier, inc=1, device_id={"row": peer(o)})
            pl.semaphore_signal(barrier, inc=1, device_id={"row": peer(o), "col": 1 - col})
        pl.semaphore_signal(barrier, inc=1, device_id={"col": 1 - col})

        cacc[...] = jnp.zeros_like(cacc)
        for b in range(ublk):
            m_copies[b].wait()

            def colsum(i, carry):
                r = pl.ds(pl.multiple_of(b * LANES + i * 32, 32), 32)
                v = m32[r, :].astype(F32)
                cacc[...] += jnp.sum(v.reshape(4, 8, items), axis=0)
                a[r, :] = v.astype(BF16)
                return carry
            lax.fori_loop(0, LANES // 32, colsum, 0)
        dsum = jnp.sum(cacc[...], axis=0, keepdims=True)
        for i in range(iblk):
            deg[me, i:i + 1, :] = dsum[:, i * LANES:(i + 1) * LANES]
        c_eu.wait()
        c_ei.wait()
        c_tr.wait()
        own0 = jnp.concatenate([ei0[...], ei0[...]], axis=1).astype(F32)
        e0p[me] = jnp.where(lo_lanes(own0[0:hs]), own0[0:hs], own0[hs:shard]).astype(BF16)
        pl.semaphore_wait(barrier, 2 * rows_n - 1)
        spread(deg.at[me], deg_s, deg_r)
        send(eu0t.at[col], eu0t.at[col], eu0_s, eu0_r, {"col": 1 - col})

        ones = jnp.ones((items, LANES), BF16)
        for b in range(ublk):
            rsum = jnp.dot(a[b * LANES:(b + 1) * LANES, :], ones, preferred_element_type=F32)
            usum[col, b:b + 1, :] = jnp.transpose(rsum)[0:1, :]
        send(usum.at[col], usum.at[col], us_s, us_r, {"col": 1 - col})
        def flip(i, carry):
            c = pl.ds(pl.multiple_of(i * LANES, LANES), LANES)
            t = jnp.transpose(a[:, c])
            n = ((i % side - my + side) % side) * side + ((i // side - mz + side) % side) * plane
            for x in range(side):
                r = pl.ds(pl.multiple_of((n + nxs[x]) * hs, hs), hs)
                at[r, 0:users] = t[x * shard:x * shard + hs]
                at[r, users:2 * users] = t[x * shard + hs:(x + 1) * shard]
            return carry
        lax.fori_loop(0, iblk, flip, 0)
        spread(e0p.at[me], e0_s, e0_r)
        trips = trip[...]
        tn = trips.shape[1]
        tq = tn // 2
        ids = lax.broadcasted_iota(jnp.int32, (users, tn), 0) + me * users
        hot[...] = jnp.transpose(jnp.where(ids == trips[0:1, :], 1.0, 0.0)).astype(BF16)
        wait_bytes(usum.at[0], us_r)
        su = lax.rsqrt(jnp.maximum(usum[0] + usum[1], 1.0))
        for b in range(ublk):
            suc[b * LANES:(b + 1) * LANES, :] = jnp.transpose(jnp.broadcast_to(su[b:b + 1, :], (LANES, LANES)))
        wait_bytes(eu0t.at[0], eu0_r)
        eu0[...] = jnp.transpose(jnp.concatenate([eu0t[0], eu0t[1]], axis=0))
        stack(eu0[...].astype(F32), w0, 0)

        wait_bytes(deg.at[others], deg_r)
        sv = lax.rsqrt(jnp.maximum(jnp.sum(deg[...], axis=0), 1.0))
        svr[...] = sv
        svt = jnp.transpose(jnp.concatenate([sv, jnp.zeros((LANES - iblk, LANES), F32)], axis=0))
        for i in range(iblk):
            t = jnp.broadcast_to(svt[:, i:i + 1], (LANES, LANES))
            n = nys[i % side] + ((i // side - mz + side) % side) * plane
            for x in range(side):
                r = pl.ds(pl.multiple_of((n + nxs[x]) * hs, hs), hs)
                svc[0, r, :] = t[x * shard:x * shard + hs]
                svc[1, r, :] = t[x * shard + hs:(x + 1) * shard]

        def scale_at(i, carry):
            r = pl.ds(pl.multiple_of(i * LANES, LANES), LANES)
            for k in range(2):
                t = svc[k, r, :]
                for b in range(ublk):
                    c = slice(k * users + b * LANES, k * users + (b + 1) * LANES)
                    at[r, c] = at[r, c] * (su[b:b + 1, :] * t).astype(BF16)
            return carry
        lax.fori_loop(0, items // 2 // LANES, scale_at, 0)

        def item_sums(w, q, r, ssem, rsem):
            for dz in sorted(range(side), key=lambda d: -far(d)):
                v = jnp.dot(at[dz * plane * hs:(dz + 1) * plane * hs, :], w[...], preferred_element_type=F32)
                q[dz * plane:(dz + 1) * plane] = v.reshape(plane, hs, LANES)
                for o in offsets:
                    if o[2] == dz:
                        send(q.at[o[0] + side * o[1] + plane * o[2]], r.at[me], ssem, rsem, {"row": peer(o)})
            r[me] = q[0]

        def user_sums(pan, up, ur, ssem, rsem):
            h = half // 2
            for k in range(2):
                r = slice(k * h, (k + 1) * h)
                lo = jnp.dot(a[k * h:(k + 1) * h, :], pan[...], preferred_element_type=F32)
                hi = jnp.dot(a[half + k * h:half + (k + 1) * h, :], pan[...], preferred_element_type=F32)
                up[r, :] = jnp.where(lo_lanes(lo), lo, hi)
                send(up.at[pl.ds(k * h, h)], ur.at[pl.ds(k * h, h)], ssem.at[k], rsem.at[k], {"col": 1 - col})

        def user_rows(up, ur, rsem, eu, w):
            h = half // 2
            for k in range(2):
                wait_bytes(ur.at[pl.ds(k * h, h)], rsem.at[k])
                s = up[k * h:(k + 1) * h, :] + ur[k * h:(k + 1) * h, :]
                eu[k * h:(k + 1) * h, :] = s.astype(BF16)
                if w is not None:
                    stack(s, w, k)

        item_sums(w0, q1, r1, r1_s, r1_r)

        def scale_a(b, carry):
            r = pl.ds(pl.multiple_of(b * LANES, LANES), LANES)
            t = suc[r, :]
            for i in range(iblk):
                c = slice(i * LANES, (i + 1) * LANES)
                a[r, c] = a[r, c] * (t * svr[i:i + 1, :]).astype(BF16)
            return carry
        lax.fori_loop(0, ublk, scale_a, 0)
        wait_bytes(e0p.at[others], e0_r)
        unpack(e0p, e0d)
        user_sums(e0d, up1, ur1, u1_s, u1_r)
        user_rows(up1, ur1, u1_r, eu1, w1)
        item_sums(w1, q2, r2, r2_s, r2_r)
        wait_bytes(r1.at[others], r1_r)
        g1[me] = jnp.sum(r1[...], axis=0).astype(BF16)
        spread(g1.at[me], g1_s, g1_r)
        wait_bytes(r2.at[others], r2_r)
        g2[me] = jnp.sum(r2[...], axis=0).astype(BF16)
        spread(g2.at[me], g2_s, g2_r)
        wait_bytes(g1.at[others], g1_r)
        unpack(g1, pan1)
        user_sums(pan1, up2, ur2, u2_s, u2_r)
        user_rows(up2, ur2, u2_r, eu2, w2)
        item_sums(w2, q3, r3, r3_s, r3_r)
        wait_bytes(g2.at[others], g2_r)
        unpack(g2, pan2)
        user_sums(pan2, up3, ur3, u3_s, u3_r)
        user_rows(up3, ur3, u3_r, eu3, None)

        t = eu0[...].astype(F32) + eu1[...].astype(F32) + eu2[...].astype(F32) + eu3[...].astype(F32)
        outp[...] = (t * 0.25).astype(BF16)
        first = jnp.dot(hot[:, 0:half], outp[...], preferred_element_type=F32)
        second = jnp.dot(hot[:, half:users], outp[...], preferred_element_type=F32)
        top = first[0:tq] + pltpu.roll(second[0:tq], DIM, 1)
        bot = pltpu.roll(first[tq:tn], DIM, 1) + second[tq:tn]
        ea[...] = jnp.where(lo_lanes(top), top, bot).astype(BF16)
        for o in (2, 1, 3):
            send(ea, ear1.at[o - 1], ea1_s.at[o - 1], ea1_r.at[o - 1], {"row": pxs[0] + pys[0] + pzs[o]})
        flat = jnp.transpose(outp[...])
        ou_hbm[...] = jnp.where(col == 0, flat[0:DIM, :], flat[DIM:2 * DIM, :])
        for o in range(1, side):
            wait_bytes(ear1.at[o - 1], ea1_r.at[o - 1])
        ea1[...] = (ea[...].astype(F32) + jnp.sum(ear1[...].astype(F32), axis=0)).astype(BF16)
        for o in offsets:
            if o[2] == 0:
                send(ea1, ear2.at[o[0] + side * o[1]], ea2_s, ea2_r, {"row": peer(o)})
        ear2[0] = ea1[...]
        g = g1[me].astype(F32)
        h = g2[me].astype(F32)
        tot = (own0 + jnp.concatenate([dup_lo(g), dup_hi(g)], axis=0)) + jnp.concatenate([dup_lo(h), dup_hi(h)], axis=0)
        rowid = lax.broadcasted_iota(jnp.int32, (shard, LANES), 0) + (col * items + me * shard)
        wait_bytes(r3.at[others], r3_r)
        s3 = jnp.sum(r3[...], axis=0).astype(BF16).astype(F32)
        oi = ((tot + jnp.concatenate([dup_lo(s3), dup_hi(s3)], axis=0)) * 0.25).astype(BF16)
        oi_hbm[...] = oi[:, 0:DIM]
        wait_bytes(ear2.at[pl.ds(0, plane - 1)], ea2_r)
        eav = jnp.sum(ear2[...].astype(F32), axis=0)
        users_v = jnp.concatenate([eav[:, 0:DIM], pltpu.roll(eav, DIM, 1)[:, 0:DIM]], axis=0).astype(BF16)

        dots = lax.dot_general(oi[:, 0:DIM], users_v, (((1,), (1,)), ((), ())), preferred_element_type=F32)
        xp = jnp.sum(jnp.where(rowid == trips[1:2, :], dots, 0.0), axis=0, keepdims=True)
        xn = jnp.sum(jnp.where(rowid == trips[2:3, :], dots, 0.0), axis=0, keepdims=True)
        mine = col * rows_n + me
        xs[mine, 0:1, :] = xp - xn
        for o in offsets:
            for c in (1 - col, col):
                send(xs.at[mine, line], xs.at[mine, line], xs_s, xs_r, {"row": peer(o), "col": c})
        send(xs.at[mine, line], xs.at[mine, line], xs_s, xs_r, {"col": 1 - col})
        wait_bytes(xs.at[pl.ds(0, 2 * rows_n - 1), line], xs_r)
        neg = -jnp.sum(xs[:, 0:1, :], axis=0)
        sp = jnp.maximum(neg, 0.0) + jnp.log1p(jnp.exp(-jnp.abs(neg)))
        loss_hbm[...] = jnp.sum(sp, axis=1, keepdims=True) * (1.0 / sp.shape[1])

        wait_bytes(deg.at[others], deg_s)
        wait_bytes(e0p.at[others], e0_s)
        wait_bytes(eu0t.at[0], eu0_s)
        wait_bytes(usum.at[0], us_s)
        for up, sem in ((up1, u1_s), (up2, u2_s), (up3, u3_s)):
            for k in range(2):
                wait_bytes(up.at[pl.ds(0, half // 2)], sem.at[k])
        wait_bytes(r1.at[others], r1_s)
        wait_bytes(r2.at[others], r2_s)
        wait_bytes(r3.at[others], r3_s)
        wait_bytes(g1.at[others], g1_s)
        wait_bytes(g2.at[others], g2_s)
        for o in range(1, side):
            wait_bytes(ea, ea1_s.at[o - 1])
        wait_bytes(ear2.at[pl.ds(0, plane - 1)], ea2_s)
        wait_bytes(xs.at[pl.ds(0, 2 * rows_n - 1), line], xs_s)

    def local_prog(mask_blk, user_shard, item_shard, triples):
        users, items = mask_blk.shape
        half, dim = user_shard.shape
        shard = item_shard.shape[0]
        trips = triples.shape[0]
        V = pltpu.VMEM
        D = pltpu.SemaphoreType.DMA
        packed = (rows_n, shard // 2, LANES)
        scratch = [
            V((users, items), jnp.int32), V((users, items), BF16), V((items // 2, 2 * users), BF16),
            V((8, items), F32), V((3, trips), jnp.int32),
            V((rows_n, items // LANES, LANES), F32), V((2, users // LANES, LANES), F32),
            V((users, LANES), F32), V((items // LANES, LANES), F32), V((2, items // 2, LANES), F32),
            V((2, dim, half), BF16), V((shard, dim), BF16), V(packed, BF16),
        ] + [V((items, LANES), BF16)] * 3 + [V((half, LANES), F32)] * 6 + [V((2 * users, LANES), BF16)] * 3 + [
            V((half, LANES), BF16)] * 4 + [V(packed, F32)] * 6 + [V(packed, BF16)] * 2 + [
            V((half, LANES), BF16), V((dim, half), BF16), V((shard, dim), BF16),
            V((trips // 2, LANES), BF16), V((side - 1, trips // 2, LANES), BF16),
            V((trips // 2, LANES), BF16), V((plane, trips // 2, LANES), BF16),
            V((2 * rows_n, 8, LANES), F32), V((1, 1), F32), V((trips, users), BF16),
            D((users // LANES,)), D((3,)), D((3,)),
        ] + [D] * 8 + [D((2,))] * 6 + [D] * 10 + [D((side - 1,))] * 2 + [D] * 4
        ANY = pl.BlockSpec(memory_space=pl.ANY)
        out_user, out_item, loss = pl.pallas_call(
            kernel,
            out_shape=(pltpu.VMEM((dim, half), BF16), pltpu.VMEM((shard, dim), BF16), pltpu.VMEM((1, 1), F32)),
            in_specs=[ANY] * 4,
            out_specs=(pl.BlockSpec(memory_space=pltpu.VMEM),) * 3,
            scratch_shapes=scratch,
            compiler_params=pltpu.CompilerParams(collective_id=0, has_side_effects=True,
                                                 vmem_limit_bytes=56 << 20),
        )(mask_blk, user_shard.T, item_shard, triples.T)
        return out_user.T, out_item, loss[0, 0]

    return jax.shard_map(local_prog, mesh=mesh, in_specs=(P("row", "col"), P(("row", "col"), None), P(("col", "row"), None), P(None, None)), out_specs=(P(("row", "col"), None), P(("col", "row"), None), P()), check_vma=False)
```

```python
import jax
import jax.numpy as jnp
from jax import lax
from jax.experimental import pallas as pl
from jax.experimental.pallas import tpu as pltpu
from jax.sharding import PartitionSpec as P

F32 = jnp.float32
BF16 = jnp.bfloat16
LANES = 128
DIM = 64


def solution(mesh):
    rows_n = mesh.shape["row"]
    side = round(rows_n ** (1 / 3))
    plane = side * side

    def far(d):
        return min(d, side - d)

    offsets = [(dx, dy, dz) for dz in range(side) for dy in range(side) for dx in range(side)]
    offsets = sorted(offsets[1:], key=lambda o: -(far(o[0]) + far(o[1]) + far(o[2])))

    def kernel(m_hbm, eu_hbm, ei_hbm, trip_hbm, ou_hbm, oi_hbm, loss_hbm,
               m32, a, at, cacc, trip, deg, usum, suc, svr, svc, eu0t, ei0, e0p, e0d, pan1, pan2,
               up1, ur1, up2, ur2, up3, ur3, w0, w1, w2, eu0, eu1, eu2, eu3, q1, q2, q3, r1, r2, t3, m3, f3, g1, g2, outp, outu, outi,
               ea, ear1, ea1, ear2, ea3, xs, lossv, hot,
               m_sem, in_sem, out_sem,
               deg_s, deg_r, e0_s, e0_r, eu0_s, eu0_r, us_s, us_r, u1_s, u1_r, u2_s, u2_r, u3_s, u3_r,
               r1_s, r1_r, r2_s, r2_r, r3_s, r3_r, g1_s, g1_r, g2_s, g2_r,
               ea1_s, ea1_r, ea2_s, ea2_r, xs_s, xs_r, f3_s, f3_r, ea3_s, ea3_r):
        me = lax.axis_index("row")
        col = lax.axis_index("col")
        mx = me % side
        my = (me // side) % side
        mz = me // plane
        pxs = [(mx + d) % side for d in range(side)]
        pys = [((my + d) % side) * side for d in range(side)]
        pzs = [((mz + d) % side) * plane for d in range(side)]
        nxs = [(d - mx + side) % side for d in range(side)]
        nys = [((d - my + side) % side) * side for d in range(side)]
        users, items = a.shape
        half = users // 2
        shard = items // rows_n
        hs = shard // 2
        ublk = users // LANES
        iblk = items // LANES
        others = pl.ds(0, rows_n - 1)
        axes3 = (0, 1)
        line = pl.ds(0, 1)

        def peer(o):
            return pxs[o[0]] + pys[o[1]] + pzs[o[2]]

        def lo_lanes(v):
            return lax.broadcasted_iota(jnp.int32, v.shape, v.ndim - 1) < DIM

        def dup_lo(v):
            return jnp.where(lo_lanes(v), v, pltpu.roll(v, DIM, v.ndim - 1))

        def dup_hi(v):
            return jnp.where(lo_lanes(v), pltpu.roll(v, DIM, v.ndim - 1), v)

        def send(src, dst, ssem, rsem, where):
            pltpu.make_async_remote_copy(src_ref=src, dst_ref=dst, send_sem=ssem, recv_sem=rsem,
                                         device_id=where).start()

        def wait_bytes(ref, sem):
            pltpu.make_async_copy(ref, ref, sem).wait()

        def spread(ref, ssem, rsem):
            for o in offsets:
                send(ref, ref, ssem, rsem, {"row": peer(o)})

        def unpack(src, dst):
            def body(i, carry):
                v = src[pl.ds(i * plane, plane)].astype(F32)
                both = jnp.concatenate([dup_lo(v), dup_hi(v)], axis=1).astype(BF16)
                dst[pl.ds(pl.multiple_of(i * plane * shard, plane * shard), plane * shard), :] = both.reshape(plane * shard, LANES)
                return carry
            lax.fori_loop(0, rows_n // plane, body, 0)

        def stack(v, w, k):
            n = v.shape[0]
            t = pltpu.roll(v, DIM, 1)
            lo = lo_lanes(v)
            for i, x in enumerate((jnp.where(lo, v, 0.0), jnp.where(lo, t, 0.0), jnp.where(lo, 0.0, t), jnp.where(lo, 0.0, v))):
                w[i * half + k * n:i * half + (k + 1) * n, :] = x.astype(BF16)

        m_copies = []
        for b in range(ublk):
            blk = pl.ds(b * LANES, LANES)
            m_copies.append(pltpu.make_async_copy(m_hbm.at[blk], m32.at[blk], m_sem.at[b]))
            m_copies[-1].start()
        c_eu = pltpu.make_async_copy(eu_hbm, eu0t.at[col], in_sem.at[0])
        c_ei = pltpu.make_async_copy(ei_hbm, ei0, in_sem.at[1])
        c_tr = pltpu.make_async_copy(trip_hbm, trip, in_sem.at[2])
        c_eu.start()
        c_ei.start()
        c_tr.start()
        barrier = pltpu.get_barrier_semaphore()
        for o in offsets:
            pl.semaphore_signal(barrier, inc=1, device_id={"row": peer(o)})
            pl.semaphore_signal(barrier, inc=1, device_id={"row": peer(o), "col": 1 - col})
        pl.semaphore_signal(barrier, inc=1, device_id={"col": 1 - col})

        cacc[...] = jnp.zeros_like(cacc)
        for b in range(ublk):
            m_copies[b].wait()

            def colsum(i, carry):
                r = pl.ds(pl.multiple_of(b * LANES + i * 32, 32), 32)
                v = m32[r, :].astype(F32)
                cacc[...] += jnp.sum(v.reshape(4, 8, items), axis=0)
                a[r, :] = v.astype(BF16)
                return carry
            lax.fori_loop(0, LANES // 32, colsum, 0)
        dsum = jnp.sum(cacc[...], axis=0, keepdims=True)
        for i in range(iblk):
            deg[me, i:i + 1, :] = dsum[:, i * LANES:(i + 1) * LANES]
        c_eu.wait()
        c_ei.wait()
        c_tr.wait()
        own0 = jnp.concatenate([ei0[...], ei0[...]], axis=1).astype(F32)
        e0p[me] = jnp.where(lo_lanes(own0[0:hs]), own0[0:hs], own0[hs:shard]).astype(BF16)
        pl.semaphore_wait(barrier, 2 * rows_n - 1)
        spread(deg.at[me], deg_s, deg_r)
        send(eu0t.at[col], eu0t.at[col], eu0_s, eu0_r, {"col": 1 - col})

        ones = jnp.ones((items, LANES), BF16)
        for b in range(ublk):
            rsum = jnp.dot(a[b * LANES:(b + 1) * LANES, :], ones, preferred_element_type=F32)
            usum[col, b:b + 1, :] = jnp.transpose(rsum)[0:1, :]
        send(usum.at[col], usum.at[col], us_s, us_r, {"col": 1 - col})
        def flip(i, carry):
            c = pl.ds(pl.multiple_of(i * LANES, LANES), LANES)
            t = jnp.transpose(a[:, c])
            n = ((i % side - my + side) % side) * side + ((i // side - mz + side) % side) * plane
            for x in range(side):
                r = pl.ds(pl.multiple_of((n + nxs[x]) * hs, hs), hs)
                at[r, 0:users] = t[x * shard:x * shard + hs]
                at[r, users:2 * users] = t[x * shard + hs:(x + 1) * shard]
            return carry
        lax.fori_loop(0, iblk, flip, 0)
        spread(e0p.at[me], e0_s, e0_r)
        trips = trip[...]
        tn = trips.shape[1]
        tq = tn // 2
        ids = lax.broadcasted_iota(jnp.int32, (users, tn), 0) + me * users
        hot[...] = jnp.transpose(jnp.where(ids == trips[0:1, :], 1.0, 0.0)).astype(BF16)
        wait_bytes(usum.at[0], us_r)
        su = lax.rsqrt(jnp.maximum(usum[0] + usum[1], 1.0))
        for b in range(ublk):
            suc[b * LANES:(b + 1) * LANES, :] = jnp.transpose(jnp.broadcast_to(su[b:b + 1, :], (LANES, LANES)))
        wait_bytes(eu0t.at[0], eu0_r)
        eu0[...] = jnp.transpose(jnp.concatenate([eu0t[0], eu0t[1]], axis=0))
        stack(eu0[...].astype(F32), w0, 0)

        wait_bytes(deg.at[others], deg_r)
        sv = lax.rsqrt(jnp.maximum(jnp.sum(deg[...], axis=0), 1.0))
        svr[...] = sv
        svt = jnp.transpose(jnp.concatenate([sv, jnp.zeros((LANES - iblk, LANES), F32)], axis=0))
        for i in range(iblk):
            t = jnp.broadcast_to(svt[:, i:i + 1], (LANES, LANES))
            n = nys[i % side] + ((i // side - mz + side) % side) * plane
            for x in range(side):
                r = pl.ds(pl.multiple_of((n + nxs[x]) * hs, hs), hs)
                svc[0, r, :] = t[x * shard:x * shard + hs]
                svc[1, r, :] = t[x * shard + hs:(x + 1) * shard]

        def scale_at(i, carry):
            r = pl.ds(pl.multiple_of(i * LANES, LANES), LANES)
            for k in range(2):
                t = svc[k, r, :]
                for b in range(ublk):
                    c = slice(k * users + b * LANES, k * users + (b + 1) * LANES)
                    at[r, c] = at[r, c] * (su[b:b + 1, :] * t).astype(BF16)
            return carry
        lax.fori_loop(0, items // 2 // LANES, scale_at, 0)

        def item_sums(w, q, r, ssem, rsem):
            for dz in sorted(range(side), key=lambda d: -far(d)):
                v = jnp.dot(at[dz * plane * hs:(dz + 1) * plane * hs, :], w[...], preferred_element_type=F32)
                q[dz * plane:(dz + 1) * plane] = v.reshape(plane, hs, LANES)
                for o in offsets:
                    if o[2] == dz:
                        send(q.at[o[0] + side * o[1] + plane * o[2]], r.at[me], ssem, rsem, {"row": peer(o)})
            r[me] = q[0]

        def axis_view(ref, axis, d, part):
            return (ref.at[:, :, d, part], ref.at[:, d, :, part], ref.at[d, :, :, part])[axis]

        def axis_peer(axis, d):
            o = [0, 0, 0]
            o[axis] = d
            return peer(o)

        def item_dots(w, q):
            for dz in range(side):
                v = jnp.dot(at[dz * plane * hs:(dz + 1) * plane * hs, :], w[...], preferred_element_type=F32)
                q[dz] = v.reshape(side, side, hs, LANES)

        def lines_start(q, axes, tmp, ssem, rsem):
            n = hs // len(axes)
            for k, axis in enumerate(axes):
                for d in sorted(range(1, side), key=lambda d: -far(d)):
                    send(axis_view(q, axis, d, pl.ds(k * n, n)), tmp.at[k, d - 1], ssem.at[k, d - 1], rsem.at[k, d - 1],
                         {"row": axis_peer(axis, d)})

        def planes_start(q, axes, tmp, mid, fin, rsem, ssem2, rsem2):
            n = hs // len(axes)
            for k, axis in enumerate(axes):
                for d in range(1, side):
                    wait_bytes(tmp.at[k, d - 1], rsem.at[k, d - 1])
                own = axis_view(q, axis, 0, pl.ds(k * n, n))[...]
                mid[k] = own + tmp[k, 0] + tmp[k, 1] + tmp[k, 2]
                for o in offsets:
                    if o[axis] == 0:
                        u, v = [o[i] for i in range(3) if i != axis]
                        send(mid.at[k, v, u], fin.at[k, v * side + u], ssem2.at[k], rsem2.at[k], {"row": peer(o)})
                fin[k, 0] = mid[k, 0, 0]

        def planes_done(axes, fin, rsem2):
            out = []
            for k in range(len(axes)):
                wait_bytes(fin.at[k, pl.ds(0, plane - 1)], rsem2.at[k])
                out.append(jnp.sum(fin[k], axis=0))
            return jnp.concatenate(out, axis=0)

        def user_sums(pan, up, ur, ssem, rsem):
            h = half // 2
            for k in range(2):
                r = slice(k * h, (k + 1) * h)
                lo = jnp.dot(a[k * h:(k + 1) * h, :], pan[...], preferred_element_type=F32)
                hi = jnp.dot(a[half + k * h:half + (k + 1) * h, :], pan[...], preferred_element_type=F32)
                up[r, :] = jnp.where(lo_lanes(lo), lo, hi)
                send(up.at[pl.ds(k * h, h)], ur.at[pl.ds(k * h, h)], ssem.at[k], rsem.at[k], {"col": 1 - col})

        def user_rows(up, ur, rsem, eu, w):
            h = half // 2
            for k in range(2):
                wait_bytes(ur.at[pl.ds(k * h, h)], rsem.at[k])
                s = up[k * h:(k + 1) * h, :] + ur[k * h:(k + 1) * h, :]
                eu[k * h:(k + 1) * h, :] = s.astype(BF16)
                if w is not None:
                    stack(s, w, k)

        item_sums(w0, q1, r1, r1_s, r1_r)

        def scale_a(b, carry):
            r = pl.ds(pl.multiple_of(b * LANES, LANES), LANES)
            t = suc[r, :]
            for i in range(iblk):
                c = slice(i * LANES, (i + 1) * LANES)
                a[r, c] = a[r, c] * (t * svr[i:i + 1, :]).astype(BF16)
            return carry
        lax.fori_loop(0, ublk, scale_a, 0)
        wait_bytes(e0p.at[others], e0_r)
        unpack(e0p, e0d)
        user_sums(e0d, up1, ur1, u1_s, u1_r)
        user_rows(up1, ur1, u1_r, eu1, w1)
        item_sums(w1, q2, r2, r2_s, r2_r)
        wait_bytes(r1.at[others], r1_r)
        g1[me] = jnp.sum(r1[...], axis=0).astype(BF16)
        spread(g1.at[me], g1_s, g1_r)
        wait_bytes(r2.at[others], r2_r)
        g2[me] = jnp.sum(r2[...], axis=0).astype(BF16)
        spread(g2.at[me], g2_s, g2_r)
        wait_bytes(g1.at[others], g1_r)
        unpack(g1, pan1)
        user_sums(pan1, up2, ur2, u2_s, u2_r)
        user_rows(up2, ur2, u2_r, eu2, w2)
        item_dots(w2, q3)
        lines_start(q3, axes3, t3, r3_s, r3_r)
        wait_bytes(g2.at[others], g2_r)
        unpack(g2, pan2)
        user_sums(pan2, up3, ur3, u3_s, u3_r)
        user_rows(up3, ur3, u3_r, eu3, None)

        t = eu0[...].astype(F32) + eu1[...].astype(F32) + eu2[...].astype(F32) + eu3[...].astype(F32)
        outp[...] = (t * 0.25).astype(BF16)
        first = jnp.dot(hot[:, 0:half], outp[...], preferred_element_type=F32)
        second = jnp.dot(hot[:, half:users], outp[...], preferred_element_type=F32)
        mine = jnp.where(col == 0, first[0:tq], first[tq:tn])
        rest = jnp.where(col == 0, second[0:tq], second[tq:tn])
        top = mine[0:tq // 2] + pltpu.roll(rest[0:tq // 2], DIM, 1)
        bot = pltpu.roll(mine[tq // 2:tq], DIM, 1) + rest[tq // 2:tq]
        ea[...] = jnp.where(lo_lanes(top), top, bot).astype(BF16)
        for o in (2, 1, 3):
            send(ea, ear1.at[o - 1], ea1_s.at[o - 1], ea1_r.at[o - 1], {"row": pxs[0] + pys[0] + pzs[o]})
        planes_start(q3, axes3, t3, m3, f3, r3_r, f3_s, f3_r)
        flat = jnp.transpose(outp[...])
        ou_hbm[...] = jnp.where(col == 0, flat[0:DIM, :], flat[DIM:2 * DIM, :])
        for o in range(1, side):
            wait_bytes(ear1.at[o - 1], ea1_r.at[o - 1])
        ea1[...] = (ea[...].astype(F32) + jnp.sum(ear1[...].astype(F32), axis=0)).astype(BF16)
        for o in offsets:
            if o[2] == 0:
                send(ea1, ear2.at[o[0] + side * o[1]], ea2_s, ea2_r, {"row": peer(o)})
        ear2[0] = ea1[...]
        g = g1[me].astype(F32)
        h = g2[me].astype(F32)
        tot = (own0 + jnp.concatenate([dup_lo(g), dup_hi(g)], axis=0)) + jnp.concatenate([dup_lo(h), dup_hi(h)], axis=0)
        rowid = lax.broadcasted_iota(jnp.int32, (shard, LANES), 0) + (col * items + me * shard)
        s3 = planes_done(axes3, f3, f3_r).astype(BF16).astype(F32)
        oi = ((tot + jnp.concatenate([dup_lo(s3), dup_hi(s3)], axis=0)) * 0.25).astype(BF16)
        oi_hbm[...] = oi[:, 0:DIM]
        wait_bytes(ear2.at[pl.ds(0, plane - 1)], ea2_r)
        ea3[col] = jnp.sum(ear2[...].astype(F32), axis=0).astype(BF16)
        send(ea3.at[col], ea3.at[col], ea3_s, ea3_r, {"col": 1 - col})
        wait_bytes(ea3.at[0], ea3_r)
        halves = []
        for c in range(2):
            v = ea3[c].astype(F32)
            halves += [v[:, 0:DIM], pltpu.roll(v, DIM, 1)[:, 0:DIM]]
        users_v = jnp.concatenate(halves, axis=0).astype(BF16)

        dots = lax.dot_general(oi[:, 0:DIM], users_v, (((1,), (1,)), ((), ())), preferred_element_type=F32)
        xp = jnp.sum(jnp.where(rowid == trips[1:2, :], dots, 0.0), axis=0, keepdims=True)
        xn = jnp.sum(jnp.where(rowid == trips[2:3, :], dots, 0.0), axis=0, keepdims=True)
        slot = col * rows_n + me
        xs[slot, 0:1, :] = xp - xn
        for o in offsets:
            for c in (1 - col, col):
                send(xs.at[slot, line], xs.at[slot, line], xs_s, xs_r, {"row": peer(o), "col": c})
        send(xs.at[slot, line], xs.at[slot, line], xs_s, xs_r, {"col": 1 - col})
        wait_bytes(xs.at[pl.ds(0, 2 * rows_n - 1), line], xs_r)
        neg = -jnp.sum(xs[:, 0:1, :], axis=0)
        sp = jnp.maximum(neg, 0.0) + jnp.log1p(jnp.exp(-jnp.abs(neg)))
        loss_hbm[...] = jnp.sum(sp, axis=1, keepdims=True) * (1.0 / sp.shape[1])

        wait_bytes(deg.at[others], deg_s)
        wait_bytes(e0p.at[others], e0_s)
        wait_bytes(eu0t.at[0], eu0_s)
        wait_bytes(usum.at[0], us_s)
        for up, sem in ((up1, u1_s), (up2, u2_s), (up3, u3_s)):
            for k in range(2):
                wait_bytes(up.at[pl.ds(0, half // 2)], sem.at[k])
        wait_bytes(r1.at[others], r1_s)
        wait_bytes(r2.at[others], r2_s)
        for k in range(2):
            for d in range(side - 1):
                wait_bytes(t3.at[k, d], r3_s.at[k, d])
            wait_bytes(f3.at[k, pl.ds(0, plane - 1)], f3_s.at[k])
        wait_bytes(g1.at[others], g1_s)
        wait_bytes(g2.at[others], g2_s)
        for o in range(1, side):
            wait_bytes(ea, ea1_s.at[o - 1])
        wait_bytes(ear2.at[pl.ds(0, plane - 1)], ea2_s)
        wait_bytes(ea3.at[0], ea3_s)
        wait_bytes(xs.at[pl.ds(0, 2 * rows_n - 1), line], xs_s)

    def local_prog(mask_blk, user_shard, item_shard, triples):
        users, items = mask_blk.shape
        half, dim = user_shard.shape
        shard = item_shard.shape[0]
        trips = triples.shape[0]
        V = pltpu.VMEM
        D = pltpu.SemaphoreType.DMA
        packed = (rows_n, shard // 2, LANES)
        cube = (side, side, side, shard // 2, LANES)
        step = (side, side, shard // 4, LANES)
        scratch = [
            V((users, items), jnp.int32), V((users, items), BF16), V((items // 2, 2 * users), BF16),
            V((8, items), F32), V((3, trips), jnp.int32),
            V((rows_n, items // LANES, LANES), F32), V((2, users // LANES, LANES), F32),
            V((users, LANES), F32), V((items // LANES, LANES), F32), V((2, items // 2, LANES), F32),
            V((2, dim, half), BF16), V((shard, dim), BF16), V(packed, BF16),
        ] + [V((items, LANES), BF16)] * 3 + [V((half, LANES), F32)] * 6 + [V((2 * users, LANES), BF16)] * 3 + [
            V((half, LANES), BF16)] * 4 + [V(packed, F32)] * 2 + [V(cube, F32)] + [V(packed, F32)] * 2 + [
            V((2, side - 1) + step, F32), V((2,) + step, F32), V((2, plane) + step[2:], F32)] + [V(packed, BF16)] * 2 + [
            V((half, LANES), BF16), V((dim, half), BF16), V((shard, dim), BF16),
            V((trips // 4, LANES), BF16), V((side - 1, trips // 4, LANES), BF16),
            V((trips // 4, LANES), BF16), V((plane, trips // 4, LANES), BF16), V((2, trips // 4, LANES), BF16),
            V((2 * rows_n, 8, LANES), F32), V((1, 1), F32), V((trips, users), BF16),
            D((users // LANES,)), D((3,)), D((3,)),
        ] + [D] * 8 + [D((2,))] * 6 + [D] * 4 + [D((2, side - 1))] * 2 + [D] * 4 + [D((side - 1,))] * 2 + [D] * 4 + [D((2,))] * 2 + [D] * 2
        ANY = pl.BlockSpec(memory_space=pl.ANY)
        out_user, out_item, loss = pl.pallas_call(
            kernel,
            out_shape=(pltpu.VMEM((dim, half), BF16), pltpu.VMEM((shard, dim), BF16), pltpu.VMEM((1, 1), F32)),
            in_specs=[ANY] * 4,
            out_specs=(pl.BlockSpec(memory_space=pltpu.VMEM),) * 3,
            scratch_shapes=scratch,
            compiler_params=pltpu.CompilerParams(collective_id=0, has_side_effects=True,
                                                 vmem_limit_bytes=56 << 20),
        )(mask_blk, user_shard.T, item_shard, triples.T)
        return out_user.T, out_item, loss[0, 0]

    return jax.shard_map(local_prog, mesh=mesh, in_specs=(P("row", "col"), P(("row", "col"), None), P(("col", "row"), None), P(None, None)), out_specs=(P(("row", "col"), None), P(("col", "row"), None), P()), check_vma=False)
```

```python
import jax
import jax.numpy as jnp
from jax import lax
from jax.experimental import pallas as pl
from jax.experimental.pallas import tpu as pltpu
from jax.sharding import PartitionSpec as P

F32 = jnp.float32
BF16 = jnp.bfloat16
LANES = 128
DIM = 64


def solution(mesh):
    rows_n = mesh.shape["row"]
    side = round(rows_n ** (1 / 3))
    plane = side * side

    def far(d):
        return min(d, side - d)

    offsets = [(dx, dy, dz) for dz in range(side) for dy in range(side) for dx in range(side)]
    offsets = sorted(offsets[1:], key=lambda o: -(far(o[0]) + far(o[1]) + far(o[2])))

    by_axis = sorted(offsets, key=lambda o: (-far(o[2]), -far(o[1]), -far(o[0])))

    def kernel(m_hbm, eu_hbm, ei_hbm, trip_hbm, ou_hbm, oi_hbm, loss_hbm,
               m32, a, at, cacc, trip, deg, usum, suc, svr, svc, eu0t, ei0, e0p, e0d, pan1, pan2,
               up1, ur1, up2, ur2, up3, ur3, w0, w1, w2, eu0, eu1, eu2, eu3, q1, q2, q3, r1, r2, t3, m3, f3, g1, g2, outp, outu, outi,
               ea, ear1, ea1, ear2, ea3, xs, lossv, hot,
               m_sem, in_sem, out_sem,
               deg_s, deg_r, e0_s, e0_r, eu0_s, eu0_r, us_s, us_r, u1_s, u1_r, u2_s, u2_r, u3_s, u3_r,
               r1_s, r1_r, r2_s, r2_r, r3_s, r3_r, g1_s, g1_r, g2_s, g2_r,
               ea1_s, ea1_r, ea2_s, ea2_r, xs_s, xs_r, f3_s, f3_r, ea3_s, ea3_r):
        me = lax.axis_index("row")
        col = lax.axis_index("col")
        mx = me % side
        my = (me // side) % side
        mz = me // plane
        pxs = [(mx + d) % side for d in range(side)]
        pys = [((my + d) % side) * side for d in range(side)]
        pzs = [((mz + d) % side) * plane for d in range(side)]
        nxs = [(d - mx + side) % side for d in range(side)]
        nys = [((d - my + side) % side) * side for d in range(side)]
        users, items = a.shape
        half = users // 2
        shard = items // rows_n
        hs = shard // 2
        ublk = users // LANES
        iblk = items // LANES
        others = pl.ds(0, rows_n - 1)
        axes3 = (0, 1)
        line = pl.ds(0, 1)

        def peer(o):
            return pxs[o[0]] + pys[o[1]] + pzs[o[2]]

        def lo_lanes(v):
            return lax.broadcasted_iota(jnp.int32, v.shape, v.ndim - 1) < DIM

        def dup_lo(v):
            return jnp.where(lo_lanes(v), v, pltpu.roll(v, DIM, v.ndim - 1))

        def dup_hi(v):
            return jnp.where(lo_lanes(v), pltpu.roll(v, DIM, v.ndim - 1), v)

        def send(src, dst, ssem, rsem, where):
            pltpu.make_async_remote_copy(src_ref=src, dst_ref=dst, send_sem=ssem, recv_sem=rsem,
                                         device_id=where).start()

        def wait_bytes(ref, sem):
            pltpu.make_async_copy(ref, ref, sem).wait()

        def spread(ref, ssem, rsem):
            for o in by_axis:
                send(ref, ref, ssem, rsem, {"row": peer(o)})

        def unpack(src, dst):
            for i in range(rows_n // plane):
                v = src[i * plane:(i + 1) * plane].astype(F32)
                both = jnp.concatenate([dup_lo(v), dup_hi(v)], axis=1).astype(BF16)
                dst[i * plane * shard:(i + 1) * plane * shard, :] = both.reshape(plane * shard, LANES)

        def stack(v, w, k):
            n = v.shape[0]
            t = pltpu.roll(v, DIM, 1)
            lo = lo_lanes(v)
            for i, x in enumerate((jnp.where(lo, v, 0.0), jnp.where(lo, t, 0.0), jnp.where(lo, 0.0, t), jnp.where(lo, 0.0, v))):
                w[i * half + k * n:i * half + (k + 1) * n, :] = x.astype(BF16)

        m_copies = []
        for b in range(ublk):
            blk = pl.ds(b * LANES, LANES)
            m_copies.append(pltpu.make_async_copy(m_hbm.at[blk], m32.at[blk], m_sem.at[b]))
            m_copies[-1].start()
        c_eu = pltpu.make_async_copy(eu_hbm, eu0t.at[col], in_sem.at[0])
        c_ei = pltpu.make_async_copy(ei_hbm, ei0, in_sem.at[1])
        c_tr = pltpu.make_async_copy(trip_hbm, trip, in_sem.at[2])
        c_eu.start()
        c_ei.start()
        c_tr.start()
        barrier = pltpu.get_barrier_semaphore()
        for o in offsets:
            pl.semaphore_signal(barrier, inc=1, device_id={"row": peer(o)})
            pl.semaphore_signal(barrier, inc=1, device_id={"row": peer(o), "col": 1 - col})
        pl.semaphore_signal(barrier, inc=1, device_id={"col": 1 - col})

        cacc[...] = jnp.zeros_like(cacc)
        for b in range(ublk):
            m_copies[b].wait()

            def colsum(i, carry):
                r = pl.ds(pl.multiple_of(b * LANES + i * 32, 32), 32)
                v = m32[r, :].astype(F32)
                cacc[...] += jnp.sum(v.reshape(4, 8, items), axis=0)
                a[r, :] = v.astype(BF16)
                return carry
            lax.fori_loop(0, LANES // 32, colsum, 0)
        dsum = jnp.sum(cacc[...], axis=0, keepdims=True)
        for i in range(iblk):
            deg[me, i:i + 1, :] = dsum[:, i * LANES:(i + 1) * LANES]
        c_eu.wait()
        c_ei.wait()
        c_tr.wait()
        own0 = jnp.concatenate([ei0[...], ei0[...]], axis=1).astype(F32)
        e0p[me] = jnp.where(lo_lanes(own0[0:hs]), own0[0:hs], own0[hs:shard]).astype(BF16)
        pl.semaphore_wait(barrier, 2 * rows_n - 1)
        spread(deg.at[me], deg_s, deg_r)
        send(eu0t.at[col], eu0t.at[col], eu0_s, eu0_r, {"col": 1 - col})

        ones = jnp.ones((items, LANES), BF16)
        for b in range(ublk):
            rsum = jnp.dot(a[b * LANES:(b + 1) * LANES, :], ones, preferred_element_type=F32)
            usum[col, b:b + 1, :] = jnp.transpose(rsum)[0:1, :]
        send(usum.at[col], usum.at[col], us_s, us_r, {"col": 1 - col})
        def flip(i, carry):
            c = pl.ds(pl.multiple_of(i * LANES, LANES), LANES)
            t = jnp.transpose(a[:, c])
            n = ((i % side - my + side) % side) * side + ((i // side - mz + side) % side) * plane
            for x in range(side):
                r = pl.ds(pl.multiple_of((n + nxs[x]) * hs, hs), hs)
                at[r, 0:users] = t[x * shard:x * shard + hs]
                at[r, users:2 * users] = t[x * shard + hs:(x + 1) * shard]
            return carry
        lax.fori_loop(0, iblk, flip, 0)
        spread(e0p.at[me], e0_s, e0_r)
        trips = trip[...]
        tn = trips.shape[1]
        tq = tn // 2
        ids = lax.broadcasted_iota(jnp.int32, (users, tn), 0) + me * users
        hot[...] = jnp.transpose(jnp.where(ids == trips[0:1, :], 1.0, 0.0)).astype(BF16)
        wait_bytes(usum.at[0], us_r)
        su = lax.rsqrt(jnp.maximum(usum[0] + usum[1], 1.0))
        for b in range(ublk):
            suc[b * LANES:(b + 1) * LANES, :] = jnp.transpose(jnp.broadcast_to(su[b:b + 1, :], (LANES, LANES)))
        wait_bytes(eu0t.at[0], eu0_r)
        eu0[...] = jnp.transpose(jnp.concatenate([eu0t[0], eu0t[1]], axis=0))
        stack(eu0[...].astype(F32), w0, 0)

        wait_bytes(deg.at[others], deg_r)
        sv = lax.rsqrt(jnp.maximum(jnp.sum(deg[...], axis=0), 1.0))
        svr[...] = sv
        svt = jnp.transpose(jnp.concatenate([sv, jnp.zeros((LANES - iblk, LANES), F32)], axis=0))
        for i in range(iblk):
            t = jnp.broadcast_to(svt[:, i:i + 1], (LANES, LANES))
            n = nys[i % side] + ((i // side - mz + side) % side) * plane
            for x in range(side):
                r = pl.ds(pl.multiple_of((n + nxs[x]) * hs, hs), hs)
                svc[0, r, :] = t[x * shard:x * shard + hs]
                svc[1, r, :] = t[x * shard + hs:(x + 1) * shard]

        def scale_at(i, carry):
            r = pl.ds(pl.multiple_of(i * LANES, LANES), LANES)
            for k in range(2):
                t = svc[k, r, :]
                for b in range(ublk):
                    c = slice(k * users + b * LANES, k * users + (b + 1) * LANES)
                    at[r, c] = at[r, c] * (su[b:b + 1, :] * t).astype(BF16)
            return carry
        lax.fori_loop(0, items // 2 // LANES, scale_at, 0)

        def item_sums(w, q, r, ssem, rsem):
            for dz in sorted(range(side), key=lambda d: -far(d)):
                v = jnp.dot(at[dz * plane * hs:(dz + 1) * plane * hs, :], w[...], preferred_element_type=F32)
                q[dz * plane:(dz + 1) * plane] = v.reshape(plane, hs, LANES)
                for o in offsets:
                    if o[2] == dz:
                        send(q.at[o[0] + side * o[1] + plane * o[2]], r.at[me], ssem, rsem, {"row": peer(o)})
            r[me] = q[0]

        def item_sums_late(w, q, r, ssem, rsem):
            for dz in range(side):
                v = jnp.dot(at[dz * plane * hs:(dz + 1) * plane * hs, :], w[...], preferred_element_type=F32)
                q[dz * plane:(dz + 1) * plane] = v.reshape(plane, hs, LANES)
            for o in by_axis:
                send(q.at[o[0] + side * o[1] + plane * o[2]], r.at[me], ssem, rsem, {"row": peer(o)})
            r[me] = q[0]

        def axis_view(ref, axis, d, part):
            return (ref.at[:, :, d, part], ref.at[:, d, :, part], ref.at[d, :, :, part])[axis]

        def axis_peer(axis, d):
            o = [0, 0, 0]
            o[axis] = d
            return peer(o)

        def item_dots(w, q):
            for dz in range(side):
                v = jnp.dot(at[dz * plane * hs:(dz + 1) * plane * hs, :], w[...], preferred_element_type=F32)
                q[dz] = v.reshape(side, side, hs, LANES)

        def lines_start(q, axes, tmp, ssem, rsem):
            n = hs // len(axes)
            for k, axis in enumerate(axes):
                for d in sorted(range(1, side), key=lambda d: -far(d)):
                    send(axis_view(q, axis, d, pl.ds(k * n, n)), tmp.at[k, d - 1], ssem.at[k, d - 1], rsem.at[k, d - 1],
                         {"row": axis_peer(axis, d)})

        def planes_start(q, axes, tmp, mid, fin, rsem, ssem2, rsem2):
            n = hs // len(axes)
            for k, axis in enumerate(axes):
                for d in range(1, side):
                    wait_bytes(tmp.at[k, d - 1], rsem.at[k, d - 1])
                own = axis_view(q, axis, 0, pl.ds(k * n, n))[...]
                mid[k] = own + tmp[k, 0] + tmp[k, 1] + tmp[k, 2]
                for o in offsets:
                    if o[axis] == 0:
                        u, v = [o[i] for i in range(3) if i != axis]
                        send(mid.at[k, v, u], fin.at[k, v * side + u], ssem2.at[k], rsem2.at[k], {"row": peer(o)})
                fin[k, 0] = mid[k, 0, 0]

        def planes_done(axes, fin, rsem2):
            out = []
            for k in range(len(axes)):
                wait_bytes(fin.at[k, pl.ds(0, plane - 1)], rsem2.at[k])
                out.append(jnp.sum(fin[k], axis=0))
            return jnp.concatenate(out, axis=0)

        def user_sums(pan, up, ur, ssem, rsem):
            h = half // 2
            for k in range(2):
                r = slice(k * h, (k + 1) * h)
                lo = jnp.dot(a[k * h:(k + 1) * h, :], pan[...], preferred_element_type=F32)
                hi = jnp.dot(a[half + k * h:half + (k + 1) * h, :], pan[...], preferred_element_type=F32)
                up[r, :] = jnp.where(lo_lanes(lo), lo, hi)
                send(up.at[pl.ds(k * h, h)], ur.at[pl.ds(k * h, h)], ssem.at[k], rsem.at[k], {"col": 1 - col})

        def user_rows(up, ur, rsem, eu, w):
            h = half // 2
            for k in range(2):
                wait_bytes(ur.at[pl.ds(k * h, h)], rsem.at[k])
                s = up[k * h:(k + 1) * h, :] + ur[k * h:(k + 1) * h, :]
                eu[k * h:(k + 1) * h, :] = s.astype(BF16)
                if w is not None:
                    stack(s, w, k)

        item_sums_late(w0, q1, r1, r1_s, r1_r)

        def scale_a(b, carry):
            r = pl.ds(pl.multiple_of(b * LANES, LANES), LANES)
            t = suc[r, :]
            for i in range(iblk):
                c = slice(i * LANES, (i + 1) * LANES)
                a[r, c] = a[r, c] * (t * svr[i:i + 1, :]).astype(BF16)
            return carry
        lax.fori_loop(0, ublk, scale_a, 0)
        wait_bytes(e0p.at[others], e0_r)
        unpack(e0p, e0d)
        user_sums(e0d, up1, ur1, u1_s, u1_r)
        user_rows(up1, ur1, u1_r, eu1, w1)
        item_sums(w1, q2, r2, r2_s, r2_r)
        wait_bytes(r1.at[others], r1_r)
        g1[me] = jnp.sum(r1[...], axis=0).astype(BF16)
        spread(g1.at[me], g1_s, g1_r)
        wait_bytes(r2.at[others], r2_r)
        g2[me] = jnp.sum(r2[...], axis=0).astype(BF16)
        spread(g2.at[me], g2_s, g2_r)
        wait_bytes(g1.at[others], g1_r)
        unpack(g1, pan1)
        user_sums(pan1, up2, ur2, u2_s, u2_r)
        user_rows(up2, ur2, u2_r, eu2, w2)
        item_dots(w2, q3)
        lines_start(q3, axes3, t3, r3_s, r3_r)
        wait_bytes(g2.at[others], g2_r)
        unpack(g2, pan2)
        user_sums(pan2, up3, ur3, u3_s, u3_r)
        user_rows(up3, ur3, u3_r, eu3, None)

        t = eu0[...].astype(F32) + eu1[...].astype(F32) + eu2[...].astype(F32) + eu3[...].astype(F32)
        outp[...] = (t * 0.25).astype(BF16)
        first = jnp.dot(hot[:, 0:half], outp[...], preferred_element_type=F32)
        second = jnp.dot(hot[:, half:users], outp[...], preferred_element_type=F32)
        mine = jnp.where(col == 0, first[0:tq], first[tq:tn])
        rest = jnp.where(col == 0, second[0:tq], second[tq:tn])
        top = mine[0:tq // 2] + pltpu.roll(rest[0:tq // 2], DIM, 1)
        bot = pltpu.roll(mine[tq // 2:tq], DIM, 1) + rest[tq // 2:tq]
        ea[...] = jnp.where(lo_lanes(top), top, bot).astype(BF16)
        for o in (2, 1, 3):
            send(ea, ear1.at[o - 1], ea1_s.at[o - 1], ea1_r.at[o - 1], {"row": pxs[0] + pys[0] + pzs[o]})
        planes_start(q3, axes3, t3, m3, f3, r3_r, f3_s, f3_r)
        flat = jnp.transpose(outp[...])
        ou_hbm[...] = jnp.where(col == 0, flat[0:DIM, :], flat[DIM:2 * DIM, :])
        for o in range(1, side):
            wait_bytes(ear1.at[o - 1], ea1_r.at[o - 1])
        ea1[...] = (ea[...].astype(F32) + jnp.sum(ear1[...].astype(F32), axis=0)).astype(BF16)
        for o in offsets:
            if o[2] == 0:
                send(ea1, ear2.at[o[0] + side * o[1]], ea2_s, ea2_r, {"row": peer(o)})
        ear2[0] = ea1[...]
        g = g1[me].astype(F32)
        h = g2[me].astype(F32)
        tot = (own0 + jnp.concatenate([dup_lo(g), dup_hi(g)], axis=0)) + jnp.concatenate([dup_lo(h), dup_hi(h)], axis=0)
        rowid = lax.broadcasted_iota(jnp.int32, (shard, LANES), 0) + (col * items + me * shard)
        s3 = planes_done(axes3, f3, f3_r).astype(BF16).astype(F32)
        oi = ((tot + jnp.concatenate([dup_lo(s3), dup_hi(s3)], axis=0)) * 0.25).astype(BF16)
        oi_hbm[...] = oi[:, 0:DIM]
        wait_bytes(ear2.at[pl.ds(0, plane - 1)], ea2_r)
        ea3[col] = jnp.sum(ear2[...].astype(F32), axis=0).astype(BF16)
        send(ea3.at[col], ea3.at[col], ea3_s, ea3_r, {"col": 1 - col})
        wait_bytes(ea3.at[0], ea3_r)
        halves = []
        for c in range(2):
            v = ea3[c].astype(F32)
            halves += [v[:, 0:DIM], pltpu.roll(v, DIM, 1)[:, 0:DIM]]
        users_v = jnp.concatenate(halves, axis=0).astype(BF16)

        dots = lax.dot_general(oi[:, 0:DIM], users_v, (((1,), (1,)), ((), ())), preferred_element_type=F32)
        xp = jnp.sum(jnp.where(rowid == trips[1:2, :], dots, 0.0), axis=0, keepdims=True)
        xn = jnp.sum(jnp.where(rowid == trips[2:3, :], dots, 0.0), axis=0, keepdims=True)
        slot = col * rows_n + me
        xs[slot, 0:1, :] = xp - xn
        for o in offsets:
            for c in (1 - col, col):
                send(xs.at[slot, line], xs.at[slot, line], xs_s, xs_r, {"row": peer(o), "col": c})
        send(xs.at[slot, line], xs.at[slot, line], xs_s, xs_r, {"col": 1 - col})
        wait_bytes(xs.at[pl.ds(0, 2 * rows_n - 1), line], xs_r)
        neg = -jnp.sum(xs[:, 0:1, :], axis=0)
        sp = jnp.maximum(neg, 0.0) + jnp.log1p(jnp.exp(-jnp.abs(neg)))
        loss_hbm[...] = jnp.sum(sp, axis=1, keepdims=True) * (1.0 / sp.shape[1])

        wait_bytes(deg.at[others], deg_s)
        wait_bytes(e0p.at[others], e0_s)
        wait_bytes(eu0t.at[0], eu0_s)
        wait_bytes(usum.at[0], us_s)
        for up, sem in ((up1, u1_s), (up2, u2_s), (up3, u3_s)):
            for k in range(2):
                wait_bytes(up.at[pl.ds(0, half // 2)], sem.at[k])
        wait_bytes(r1.at[others], r1_s)
        wait_bytes(r2.at[others], r2_s)
        for k in range(2):
            for d in range(side - 1):
                wait_bytes(t3.at[k, d], r3_s.at[k, d])
            wait_bytes(f3.at[k, pl.ds(0, plane - 1)], f3_s.at[k])
        wait_bytes(g1.at[others], g1_s)
        wait_bytes(g2.at[others], g2_s)
        for o in range(1, side):
            wait_bytes(ea, ea1_s.at[o - 1])
        wait_bytes(ear2.at[pl.ds(0, plane - 1)], ea2_s)
        wait_bytes(ea3.at[0], ea3_s)
        wait_bytes(xs.at[pl.ds(0, 2 * rows_n - 1), line], xs_s)

    def local_prog(mask_blk, user_shard, item_shard, triples):
        users, items = mask_blk.shape
        half, dim = user_shard.shape
        shard = item_shard.shape[0]
        trips = triples.shape[0]
        V = pltpu.VMEM
        D = pltpu.SemaphoreType.DMA
        packed = (rows_n, shard // 2, LANES)
        cube = (side, side, side, shard // 2, LANES)
        step = (side, side, shard // 4, LANES)
        scratch = [
            V((users, items), jnp.int32), V((users, items), BF16), V((items // 2, 2 * users), BF16),
            V((8, items), F32), V((3, trips), jnp.int32),
            V((rows_n, items // LANES, LANES), F32), V((2, users // LANES, LANES), F32),
            V((users, LANES), F32), V((items // LANES, LANES), F32), V((2, items // 2, LANES), F32),
            V((2, dim, half), BF16), V((shard, dim), BF16), V(packed, BF16),
        ] + [V((items, LANES), BF16)] * 3 + [V((half, LANES), F32)] * 6 + [V((2 * users, LANES), BF16)] * 3 + [
            V((half, LANES), BF16)] * 4 + [V(packed, F32)] * 2 + [V(cube, F32)] + [V(packed, F32)] * 2 + [
            V((2, side - 1) + step, F32), V((2,) + step, F32), V((2, plane) + step[2:], F32)] + [V(packed, BF16)] * 2 + [
            V((half, LANES), BF16), V((dim, half), BF16), V((shard, dim), BF16),
            V((trips // 4, LANES), BF16), V((side - 1, trips // 4, LANES), BF16),
            V((trips // 4, LANES), BF16), V((plane, trips // 4, LANES), BF16), V((2, trips // 4, LANES), BF16),
            V((2 * rows_n, 8, LANES), F32), V((1, 1), F32), V((trips, users), BF16),
            D((users // LANES,)), D((3,)), D((3,)),
        ] + [D] * 8 + [D((2,))] * 6 + [D] * 4 + [D((2, side - 1))] * 2 + [D] * 4 + [D((side - 1,))] * 2 + [D] * 4 + [D((2,))] * 2 + [D] * 2
        ANY = pl.BlockSpec(memory_space=pl.ANY)
        out_user, out_item, loss = pl.pallas_call(
            kernel,
            out_shape=(pltpu.VMEM((dim, half), BF16), pltpu.VMEM((shard, dim), BF16), pltpu.VMEM((1, 1), F32)),
            in_specs=[ANY] * 4,
            out_specs=(pl.BlockSpec(memory_space=pltpu.VMEM),) * 3,
            scratch_shapes=scratch,
            compiler_params=pltpu.CompilerParams(collective_id=0, has_side_effects=True,
                                                 vmem_limit_bytes=56 << 20),
        )(mask_blk, user_shard.T, item_shard, triples.T)
        return out_user.T, out_item, loss[0, 0]

    return jax.shard_map(local_prog, mesh=mesh, in_specs=(P("row", "col"), P(("row", "col"), None), P(("col", "row"), None), P(None, None)), out_specs=(P(("row", "col"), None), P(("col", "row"), None), P()), check_vma=False)
```

```python
import jax
import jax.numpy as jnp
from jax import lax
from jax.experimental import pallas as pl
from jax.experimental.pallas import tpu as pltpu
from jax.sharding import PartitionSpec as P

F32 = jnp.float32
BF16 = jnp.bfloat16
LANES = 128
DIM = 64


def solution(mesh):
    rows_n = mesh.shape["row"]
    side = round(rows_n ** (1 / 3))
    plane = side * side

    def far(d):
        return min(d, side - d)

    offsets = [(dx, dy, dz) for dz in range(side) for dy in range(side) for dx in range(side)]
    offsets = sorted(offsets[1:], key=lambda o: -(far(o[0]) + far(o[1]) + far(o[2])))

    by_axis = sorted(offsets, key=lambda o: (-far(o[2]), -far(o[1]), -far(o[0])))

    def kernel(m_hbm, eu_hbm, ei_hbm, trip_hbm, ou_hbm, oi_hbm, loss_hbm,
               m32, a, at, cacc, trip, deg, usum, suc, svr, svc, eu0t, ei0, e0p, e0d, pan1, pan2,
               up1, ur1, up2, ur2, up3, ur3, w0, w1, w2, eu0, eu1, eu2, eu3, q1, q2, q3, r1, r2, t3, m3, f3, g1, g2, outp, outu, outi,
               ea, ear1, ea1, ear2, ea3, xs, lossv, hot,
               m_sem, in_sem, out_sem,
               deg_s, deg_r, e0_s, e0_r, eu0_s, eu0_r, us_s, us_r, u1_s, u1_r, u2_s, u2_r, u3_s, u3_r,
               r1_s, r1_r, r2_s, r2_r, r3_s, r3_r, g1_s, g1_r, g2_s, g2_r,
               ea1_s, ea1_r, ea2_s, ea2_r, xs_s, xs_r, f3_s, f3_r, ea3_s, ea3_r):
        me = lax.axis_index("row")
        col = lax.axis_index("col")
        mx = me % side
        my = (me // side) % side
        mz = me // plane
        pxs = [(mx + d) % side for d in range(side)]
        pys = [((my + d) % side) * side for d in range(side)]
        pzs = [((mz + d) % side) * plane for d in range(side)]
        nxs = [(d - mx + side) % side for d in range(side)]
        nys = [((d - my + side) % side) * side for d in range(side)]
        users, items = a.shape
        half = users // 2
        shard = items // rows_n
        hs = shard // 2
        ublk = users // LANES
        iblk = items // LANES
        others = pl.ds(0, rows_n - 1)
        axes3 = (0, 1)
        line = pl.ds(0, 1)

        def peer(o):
            return pxs[o[0]] + pys[o[1]] + pzs[o[2]]

        def lo_lanes(v):
            return lax.broadcasted_iota(jnp.int32, v.shape, v.ndim - 1) < DIM

        def dup_lo(v):
            return jnp.where(lo_lanes(v), v, pltpu.roll(v, DIM, v.ndim - 1))

        def dup_hi(v):
            return jnp.where(lo_lanes(v), pltpu.roll(v, DIM, v.ndim - 1), v)

        def send(src, dst, ssem, rsem, where):
            pltpu.make_async_remote_copy(src_ref=src, dst_ref=dst, send_sem=ssem, recv_sem=rsem,
                                         device_id=where).start()

        def wait_bytes(ref, sem):
            pltpu.make_async_copy(ref, ref, sem).wait()

        def spread(ref, ssem, rsem):
            for o in by_axis:
                send(ref, ref, ssem, rsem, {"row": peer(o)})

        def unpack(src, dst):
            for i in range(rows_n // plane):
                v = src[i * plane:(i + 1) * plane].astype(F32)
                both = jnp.concatenate([dup_lo(v), dup_hi(v)], axis=1).astype(BF16)
                dst[i * plane * shard:(i + 1) * plane * shard, :] = both.reshape(plane * shard, LANES)

        def stack(v, w, k):
            n = v.shape[0]
            t = pltpu.roll(v, DIM, 1)
            lo = lo_lanes(v)
            for i, x in enumerate((jnp.where(lo, v, 0.0), jnp.where(lo, t, 0.0), jnp.where(lo, 0.0, t), jnp.where(lo, 0.0, v))):
                w[i * half + k * n:i * half + (k + 1) * n, :] = x.astype(BF16)

        m_copies = []
        for b in range(ublk):
            blk = pl.ds(b * LANES, LANES)
            m_copies.append(pltpu.make_async_copy(m_hbm.at[blk], m32.at[blk], m_sem.at[b]))
            m_copies[-1].start()
        c_eu = pltpu.make_async_copy(eu_hbm, eu0t.at[col], in_sem.at[0])
        c_ei = pltpu.make_async_copy(ei_hbm, ei0, in_sem.at[1])
        c_tr = pltpu.make_async_copy(trip_hbm, trip, in_sem.at[2])
        c_eu.start()
        c_ei.start()
        c_tr.start()
        barrier = pltpu.get_barrier_semaphore()
        for o in offsets:
            pl.semaphore_signal(barrier, inc=1, device_id={"row": peer(o)})
            pl.semaphore_signal(barrier, inc=1, device_id={"row": peer(o), "col": 1 - col})
        pl.semaphore_signal(barrier, inc=1, device_id={"col": 1 - col})

        cacc[...] = jnp.zeros_like(cacc)
        for b in range(ublk):
            m_copies[b].wait()

            def colsum(i, carry):
                r = pl.ds(pl.multiple_of(b * LANES + i * 32, 32), 32)
                v = m32[r, :].astype(F32)
                cacc[...] += jnp.sum(v.reshape(4, 8, items), axis=0)
                a[r, :] = v.astype(BF16)
                return carry
            lax.fori_loop(0, LANES // 32, colsum, 0)
        dsum = jnp.sum(cacc[...], axis=0, keepdims=True)
        for i in range(iblk):
            deg[me, i:i + 1, :] = dsum[:, i * LANES:(i + 1) * LANES]
        c_eu.wait()
        c_ei.wait()
        c_tr.wait()
        own0 = jnp.concatenate([ei0[...], ei0[...]], axis=1).astype(F32)
        e0p[me] = jnp.where(lo_lanes(own0[0:hs]), own0[0:hs], own0[hs:shard]).astype(BF16)
        pl.semaphore_wait(barrier, 2 * rows_n - 1)
        spread(deg.at[me], deg_s, deg_r)
        send(eu0t.at[col], eu0t.at[col], eu0_s, eu0_r, {"col": 1 - col})

        ones = jnp.ones((items, LANES), BF16)
        for b in range(ublk):
            rsum = jnp.dot(a[b * LANES:(b + 1) * LANES, :], ones, preferred_element_type=F32)
            usum[col, b:b + 1, :] = jnp.transpose(rsum)[0:1, :]
        send(usum.at[col], usum.at[col], us_s, us_r, {"col": 1 - col})
        def flip(i, carry):
            c = pl.ds(pl.multiple_of(i * LANES, LANES), LANES)
            t = jnp.transpose(a[:, c])
            n = ((i % side - my + side) % side) * side + ((i // side - mz + side) % side) * plane
            for x in range(side):
                r = pl.ds(pl.multiple_of((n + nxs[x]) * hs, hs), hs)
                at[r, 0:users] = t[x * shard:x * shard + hs]
                at[r, users:2 * users] = t[x * shard + hs:(x + 1) * shard]
            return carry
        lax.fori_loop(0, iblk, flip, 0)
        spread(e0p.at[me], e0_s, e0_r)
        trips = trip[...]
        tn = trips.shape[1]
        tq = tn // 2
        ids = lax.broadcasted_iota(jnp.int32, (users, tn), 0) + me * users
        hot[...] = jnp.transpose(jnp.where(ids == trips[0:1, :], 1.0, 0.0)).astype(BF16)
        wait_bytes(usum.at[0], us_r)
        su = lax.rsqrt(jnp.maximum(usum[0] + usum[1], 1.0))
        for b in range(ublk):
            suc[b * LANES:(b + 1) * LANES, :] = jnp.transpose(jnp.broadcast_to(su[b:b + 1, :], (LANES, LANES)))
        wait_bytes(eu0t.at[0], eu0_r)
        eu0[...] = jnp.transpose(jnp.concatenate([eu0t[0], eu0t[1]], axis=0))
        stack(eu0[...].astype(F32), w0, 0)

        wait_bytes(deg.at[others], deg_r)
        sv = lax.rsqrt(jnp.maximum(jnp.sum(deg[...], axis=0), 1.0))
        svr[...] = sv
        svt = jnp.transpose(jnp.concatenate([sv, jnp.zeros((LANES - iblk, LANES), F32)], axis=0))
        for i in range(iblk):
            t = jnp.broadcast_to(svt[:, i:i + 1], (LANES, LANES))
            n = nys[i % side] + ((i // side - mz + side) % side) * plane
            for x in range(side):
                r = pl.ds(pl.multiple_of((n + nxs[x]) * hs, hs), hs)
                svc[0, r, :] = t[x * shard:x * shard + hs]
                svc[1, r, :] = t[x * shard + hs:(x + 1) * shard]

        def scale_at(i, carry):
            r = pl.ds(pl.multiple_of(i * LANES, LANES), LANES)
            for k in range(2):
                t = svc[k, r, :]
                for b in range(ublk):
                    c = slice(k * users + b * LANES, k * users + (b + 1) * LANES)
                    at[r, c] = at[r, c] * (su[b:b + 1, :] * t).astype(BF16)
            return carry
        lax.fori_loop(0, items // 2 // LANES, scale_at, 0)

        def item_sums(w, q, r, ssem, rsem):
            for dz in sorted(range(side), key=lambda d: -far(d)):
                v = jnp.dot(at[dz * plane * hs:(dz + 1) * plane * hs, :], w[...], preferred_element_type=F32)
                q[dz * plane:(dz + 1) * plane] = v.reshape(plane, hs, LANES)
                for o in by_axis:
                    if o[2] == dz:
                        send(q.at[o[0] + side * o[1] + plane * o[2]], r.at[me], ssem, rsem, {"row": peer(o)})
            r[me] = q[0]

        def item_sums_late(w, q, r, ssem, rsem):
            for dz in range(side):
                v = jnp.dot(at[dz * plane * hs:(dz + 1) * plane * hs, :], w[...], preferred_element_type=F32)
                q[dz * plane:(dz + 1) * plane] = v.reshape(plane, hs, LANES)
            for o in by_axis:
                send(q.at[o[0] + side * o[1] + plane * o[2]], r.at[me], ssem, rsem, {"row": peer(o)})
            r[me] = q[0]

        def axis_view(ref, axis, d, part):
            return (ref.at[:, :, d, part], ref.at[:, d, :, part], ref.at[d, :, :, part])[axis]

        def axis_peer(axis, d):
            o = [0, 0, 0]
            o[axis] = d
            return peer(o)

        def item_dots(w, q):
            for dz in range(side):
                v = jnp.dot(at[dz * plane * hs:(dz + 1) * plane * hs, :], w[...], preferred_element_type=F32)
                q[dz] = v.reshape(side, side, hs, LANES)

        def lines_start(q, axes, tmp, ssem, rsem):
            n = hs // len(axes)
            for k, axis in enumerate(axes):
                for d in sorted(range(1, side), key=lambda d: -far(d)):
                    send(axis_view(q, axis, d, pl.ds(k * n, n)), tmp.at[k, d - 1], ssem.at[k, d - 1], rsem.at[k, d - 1],
                         {"row": axis_peer(axis, d)})

        def planes_start(q, axes, tmp, mid, fin, rsem, ssem2, rsem2):
            n = hs // len(axes)
            for k, axis in enumerate(axes):
                for d in range(1, side):
                    wait_bytes(tmp.at[k, d - 1], rsem.at[k, d - 1])
                own = axis_view(q, axis, 0, pl.ds(k * n, n))[...]
                mid[k] = own + tmp[k, 0] + tmp[k, 1] + tmp[k, 2]
                for o in offsets:
                    if o[axis] == 0:
                        u, v = [o[i] for i in range(3) if i != axis]
                        send(mid.at[k, v, u], fin.at[k, v * side + u], ssem2.at[k], rsem2.at[k], {"row": peer(o)})
                fin[k, 0] = mid[k, 0, 0]

        def planes_done(axes, fin, rsem2):
            out = []
            for k in range(len(axes)):
                wait_bytes(fin.at[k, pl.ds(0, plane - 1)], rsem2.at[k])
                out.append(jnp.sum(fin[k], axis=0))
            return jnp.concatenate(out, axis=0)

        def user_sums(pan, up, ur, ssem, rsem):
            h = half // 2
            for k in range(2):
                r = slice(k * h, (k + 1) * h)
                lo = jnp.dot(a[k * h:(k + 1) * h, :], pan[...], preferred_element_type=F32)
                hi = jnp.dot(a[half + k * h:half + (k + 1) * h, :], pan[...], preferred_element_type=F32)
                up[r, :] = jnp.where(lo_lanes(lo), lo, hi)
                send(up.at[pl.ds(k * h, h)], ur.at[pl.ds(k * h, h)], ssem.at[k], rsem.at[k], {"col": 1 - col})

        def user_rows(up, ur, rsem, eu, w):
            h = half // 2
            for k in range(2):
                wait_bytes(ur.at[pl.ds(k * h, h)], rsem.at[k])
                s = up[k * h:(k + 1) * h, :] + ur[k * h:(k + 1) * h, :]
                eu[k * h:(k + 1) * h, :] = s.astype(BF16)
                if w is not None:
                    stack(s, w, k)

        item_sums_late(w0, q1, r1, r1_s, r1_r)

        def scale_a(b, carry):
            r = pl.ds(pl.multiple_of(b * LANES, LANES), LANES)
            t = suc[r, :]
            for i in range(iblk):
                c = slice(i * LANES, (i + 1) * LANES)
                a[r, c] = a[r, c] * (t * svr[i:i + 1, :]).astype(BF16)
            return carry
        lax.fori_loop(0, ublk, scale_a, 0)
        wait_bytes(e0p.at[others], e0_r)
        unpack(e0p, e0d)
        user_sums(e0d, up1, ur1, u1_s, u1_r)
        user_rows(up1, ur1, u1_r, eu1, w1)
        item_sums(w1, q2, r2, r2_s, r2_r)
        wait_bytes(r1.at[others], r1_r)
        g1[me] = jnp.sum(r1[...], axis=0).astype(BF16)
        spread(g1.at[me], g1_s, g1_r)
        wait_bytes(r2.at[others], r2_r)
        g2[me] = jnp.sum(r2[...], axis=0).astype(BF16)
        spread(g2.at[me], g2_s, g2_r)
        wait_bytes(g1.at[others], g1_r)
        unpack(g1, pan1)
        user_sums(pan1, up2, ur2, u2_s, u2_r)
        user_rows(up2, ur2, u2_r, eu2, w2)
        item_dots(w2, q3)
        lines_start(q3, axes3, t3, r3_s, r3_r)
        wait_bytes(g2.at[others], g2_r)
        unpack(g2, pan2)
        user_sums(pan2, up3, ur3, u3_s, u3_r)
        user_rows(up3, ur3, u3_r, eu3, None)

        t = eu0[...].astype(F32) + eu1[...].astype(F32) + eu2[...].astype(F32) + eu3[...].astype(F32)
        outp[...] = (t * 0.25).astype(BF16)
        first = jnp.dot(hot[:, 0:half], outp[...], preferred_element_type=F32)
        second = jnp.dot(hot[:, half:users], outp[...], preferred_element_type=F32)
        mine = jnp.where(col == 0, first[0:tq], first[tq:tn])
        rest = jnp.where(col == 0, second[0:tq], second[tq:tn])
        top = mine[0:tq // 2] + pltpu.roll(rest[0:tq // 2], DIM, 1)
        bot = pltpu.roll(mine[tq // 2:tq], DIM, 1) + rest[tq // 2:tq]
        ea[...] = jnp.where(lo_lanes(top), top, bot).astype(BF16)
        for o in (2, 1, 3):
            send(ea, ear1.at[o - 1], ea1_s.at[o - 1], ea1_r.at[o - 1], {"row": pxs[0] + pys[0] + pzs[o]})
        planes_start(q3, axes3, t3, m3, f3, r3_r, f3_s, f3_r)
        flat = jnp.transpose(outp[...])
        ou_hbm[...] = jnp.where(col == 0, flat[0:DIM, :], flat[DIM:2 * DIM, :])
        for o in range(1, side):
            wait_bytes(ear1.at[o - 1], ea1_r.at[o - 1])
        ea1[...] = (ea[...].astype(F32) + jnp.sum(ear1[...].astype(F32), axis=0)).astype(BF16)
        for o in offsets:
            if o[2] == 0:
                send(ea1, ear2.at[o[0] + side * o[1]], ea2_s, ea2_r, {"row": peer(o)})
        ear2[0] = ea1[...]
        g = g1[me].astype(F32)
        h = g2[me].astype(F32)
        tot = (own0 + jnp.concatenate([dup_lo(g), dup_hi(g)], axis=0)) + jnp.concatenate([dup_lo(h), dup_hi(h)], axis=0)
        rowid = lax.broadcasted_iota(jnp.int32, (shard, LANES), 0) + (col * items + me * shard)
        s3 = planes_done(axes3, f3, f3_r).astype(BF16).astype(F32)
        oi = ((tot + jnp.concatenate([dup_lo(s3), dup_hi(s3)], axis=0)) * 0.25).astype(BF16)
        oi_hbm[...] = oi[:, 0:DIM]
        wait_bytes(ear2.at[pl.ds(0, plane - 1)], ea2_r)
        ea3[col] = jnp.sum(ear2[...].astype(F32), axis=0).astype(BF16)
        send(ea3.at[col], ea3.at[col], ea3_s, ea3_r, {"col": 1 - col})
        wait_bytes(ea3.at[0], ea3_r)
        halves = []
        for c in range(2):
            v = ea3[c].astype(F32)
            halves += [v[:, 0:DIM], pltpu.roll(v, DIM, 1)[:, 0:DIM]]
        users_v = jnp.concatenate(halves, axis=0).astype(BF16)

        dots = lax.dot_general(oi[:, 0:DIM], users_v, (((1,), (1,)), ((), ())), preferred_element_type=F32)
        xp = jnp.sum(jnp.where(rowid == trips[1:2, :], dots, 0.0), axis=0, keepdims=True)
        xn = jnp.sum(jnp.where(rowid == trips[2:3, :], dots, 0.0), axis=0, keepdims=True)
        slot = col * rows_n + me
        xs[slot, 0:1, :] = xp - xn
        for o in offsets:
            for c in (1 - col, col):
                send(xs.at[slot, line], xs.at[slot, line], xs_s, xs_r, {"row": peer(o), "col": c})
        send(xs.at[slot, line], xs.at[slot, line], xs_s, xs_r, {"col": 1 - col})
        wait_bytes(xs.at[pl.ds(0, 2 * rows_n - 1), line], xs_r)
        neg = -jnp.sum(xs[:, 0:1, :], axis=0)
        sp = jnp.maximum(neg, 0.0) + jnp.log1p(jnp.exp(-jnp.abs(neg)))
        loss_hbm[...] = jnp.sum(sp, axis=1, keepdims=True) * (1.0 / sp.shape[1])

        wait_bytes(deg.at[others], deg_s)
        wait_bytes(e0p.at[others], e0_s)
        wait_bytes(eu0t.at[0], eu0_s)
        wait_bytes(usum.at[0], us_s)
        for up, sem in ((up1, u1_s), (up2, u2_s), (up3, u3_s)):
            for k in range(2):
                wait_bytes(up.at[pl.ds(0, half // 2)], sem.at[k])
        wait_bytes(r1.at[others], r1_s)
        wait_bytes(r2.at[others], r2_s)
        for k in range(2):
            for d in range(side - 1):
                wait_bytes(t3.at[k, d], r3_s.at[k, d])
            wait_bytes(f3.at[k, pl.ds(0, plane - 1)], f3_s.at[k])
        wait_bytes(g1.at[others], g1_s)
        wait_bytes(g2.at[others], g2_s)
        for o in range(1, side):
            wait_bytes(ea, ea1_s.at[o - 1])
        wait_bytes(ear2.at[pl.ds(0, plane - 1)], ea2_s)
        wait_bytes(ea3.at[0], ea3_s)
        wait_bytes(xs.at[pl.ds(0, 2 * rows_n - 1), line], xs_s)

    def local_prog(mask_blk, user_shard, item_shard, triples):
        users, items = mask_blk.shape
        half, dim = user_shard.shape
        shard = item_shard.shape[0]
        trips = triples.shape[0]
        V = pltpu.VMEM
        D = pltpu.SemaphoreType.DMA
        packed = (rows_n, shard // 2, LANES)
        cube = (side, side, side, shard // 2, LANES)
        step = (side, side, shard // 4, LANES)
        scratch = [
            V((users, items), jnp.int32), V((users, items), BF16), V((items // 2, 2 * users), BF16),
            V((8, items), F32), V((3, trips), jnp.int32),
            V((rows_n, items // LANES, LANES), F32), V((2, users // LANES, LANES), F32),
            V((users, LANES), F32), V((items // LANES, LANES), F32), V((2, items // 2, LANES), F32),
            V((2, dim, half), BF16), V((shard, dim), BF16), V(packed, BF16),
        ] + [V((items, LANES), BF16)] * 3 + [V((half, LANES), F32)] * 6 + [V((2 * users, LANES), BF16)] * 3 + [
            V((half, LANES), BF16)] * 4 + [V(packed, F32)] * 2 + [V(cube, F32)] + [V(packed, F32)] * 2 + [
            V((2, side - 1) + step, F32), V((2,) + step, F32), V((2, plane) + step[2:], F32)] + [V(packed, BF16)] * 2 + [
            V((half, LANES), BF16), V((dim, half), BF16), V((shard, dim), BF16),
            V((trips // 4, LANES), BF16), V((side - 1, trips // 4, LANES), BF16),
            V((trips // 4, LANES), BF16), V((plane, trips // 4, LANES), BF16), V((2, trips // 4, LANES), BF16),
            V((2 * rows_n, 8, LANES), F32), V((1, 1), F32), V((trips, users), BF16),
            D((users // LANES,)), D((3,)), D((3,)),
        ] + [D] * 8 + [D((2,))] * 6 + [D] * 4 + [D((2, side - 1))] * 2 + [D] * 4 + [D((side - 1,))] * 2 + [D] * 4 + [D((2,))] * 2 + [D] * 2
        ANY = pl.BlockSpec(memory_space=pl.ANY)
        out_user, out_item, loss = pl.pallas_call(
            kernel,
            out_shape=(pltpu.VMEM((dim, half), BF16), pltpu.VMEM((shard, dim), BF16), pltpu.VMEM((1, 1), F32)),
            in_specs=[ANY] * 4,
            out_specs=(pl.BlockSpec(memory_space=pltpu.VMEM),) * 3,
            scratch_shapes=scratch,
            compiler_params=pltpu.CompilerParams(collective_id=0, has_side_effects=True,
                                                 vmem_limit_bytes=56 << 20),
        )(mask_blk, user_shard.T, item_shard, triples.T)
        return out_user.T, out_item, loss[0, 0]

    return jax.shard_map(local_prog, mesh=mesh, in_specs=(P("row", "col"), P(("row", "col"), None), P(("col", "row"), None), P(None, None)), out_specs=(P(("row", "col"), None), P(("col", "row"), None), P()), check_vma=False)
```
